8 devices in a mesh: data: 8 (over z, y, x, core).
Axes of the slice: x: 2, y: 2, z: 1, core: 2. Of those that a mesh axis runs over, the one named last changes fastest.
Arguments:
- z_one: bfloat16 [1024, 128], P('data')
- z_two: bfloat16 [1024, 128], P('data')
- protos: bfloat16 [1000, 128], replicated
- queue_one: bfloat16 [4096, 128], P('data')
- queue_two: bfloat16 [4096, 128], P('data')
Outputs:
- output 1: float32 [1024, 1000], P('data')
- output 2: float32 [1024, 1000], P('data')
- output 3: float32 [], replicated
- output 4: float32 [1024, 128], P('data')
- output 5: float32 [1024, 128], P('data')
- output 6: float32 [1000, 128], replicated
All inputs are finite; a program needn't handle non-finite values.
Results may differ from the reference program's by a relative error of at most 0.001.
Values are sent between devices in bfloat16 or wider.
A program may use at most 1 GiB of HBM per device.

```python
import jax
import jax.numpy as jnp
from jax import lax

PROTOS = 1000
EMBED_DIM = 128
GROUP_SIZE = 8
ROWS_DEV = 128
QUEUE_DEV = 512
SINKHORN_ITERS = 3
EPSILON = 0.05
TEMPERATURE = 0.1


def unit_rows(values):
    return values / jnp.sqrt(jnp.sum(values * values, axis=-1, keepdims=True))


def setup_inputs(seed: int = 0) -> dict:
    key_list = jax.random.split(jax.random.key(seed), 8)
    noise_scale = EMBED_DIM ** -0.5
    batch_shape = (GROUP_SIZE, ROWS_DEV, EMBED_DIM)
    queue_shape = (GROUP_SIZE, QUEUE_DEV, EMBED_DIM)
    centers = unit_rows(jax.random.normal(key_list[0], (GROUP_SIZE, 1, EMBED_DIM), jnp.float32))
    queue_centers = unit_rows(jax.random.normal(key_list[1], (GROUP_SIZE, 1, EMBED_DIM), jnp.float32))
    base_rows = 1.5 * centers + noise_scale * jax.random.normal(key_list[2], batch_shape, jnp.float32)
    view_one = unit_rows(base_rows + 0.5 * noise_scale * jax.random.normal(key_list[3], batch_shape, jnp.float32))
    view_two = unit_rows(base_rows + 0.5 * noise_scale * jax.random.normal(key_list[4], batch_shape, jnp.float32))
    queue_one = unit_rows(1.5 * queue_centers + noise_scale * jax.random.normal(key_list[5], queue_shape, jnp.float32))
    queue_two = unit_rows(1.5 * queue_centers + noise_scale * jax.random.normal(key_list[6], queue_shape, jnp.float32))
    protos = unit_rows(jax.random.normal(key_list[7], (PROTOS, EMBED_DIM), jnp.float32))
    return {
        "z_one": view_one.reshape(GROUP_SIZE * ROWS_DEV, EMBED_DIM).astype(jnp.bfloat16),
        "z_two": view_two.reshape(GROUP_SIZE * ROWS_DEV, EMBED_DIM).astype(jnp.bfloat16),
        "protos": protos.astype(jnp.bfloat16),
        "queue_one": queue_one.reshape(GROUP_SIZE * QUEUE_DEV, EMBED_DIM).astype(jnp.bfloat16),
        "queue_two": queue_two.reshape(GROUP_SIZE * QUEUE_DEV, EMBED_DIM).astype(jnp.bfloat16),
    }


def scores_of(row_block, protos):
    return jnp.dot(row_block, protos.T, preferred_element_type=jnp.float32)


def scaled_col_sum(blocks, protos, col_scale, total_rows):
    def pass_body(col_acc, row_block):
        transport = jnp.exp(scores_of(row_block, protos) / EPSILON)
        row_scale = 1.0 / (total_rows * jnp.sum(transport * col_scale, axis=1))
        return col_acc + jnp.sum(transport * row_scale[:, None], axis=0), None
    col_sum, _ = lax.scan(pass_body, jnp.zeros((PROTOS,), jnp.float32), blocks)
    return col_sum


def column_scale(blocks, protos):
    total_rows = GROUP_SIZE * (ROWS_DEV + QUEUE_DEV)

    def first_body(col_acc, row_block):
        transport = jnp.exp(scores_of(row_block, protos) / EPSILON)
        return col_acc + jnp.sum(transport, axis=0), None

    col_sum, _ = lax.scan(first_body, jnp.zeros((PROTOS,), jnp.float32), blocks)
    col_scale = 1.0 / (PROTOS * col_sum)
    for _ in range(SINKHORN_ITERS - 1):
        col_scale = 1.0 / (PROTOS * scaled_col_sum(blocks, protos, col_scale, total_rows))
    return col_scale


def reference(z_one, z_two, protos, queue_one, queue_two):
    batch_one = z_one.reshape(GROUP_SIZE, ROWS_DEV, EMBED_DIM)
    batch_two = z_two.reshape(GROUP_SIZE, ROWS_DEV, EMBED_DIM)
    rows_all_one = jnp.concatenate([batch_one, queue_one.reshape(GROUP_SIZE, QUEUE_DEV, EMBED_DIM)], axis=1)
    rows_all_two = jnp.concatenate([batch_two, queue_two.reshape(GROUP_SIZE, QUEUE_DEV, EMBED_DIM)], axis=1)
    scale_one = column_scale(rows_all_one, protos)
    scale_two = column_scale(rows_all_two, protos)
    batch_total = GROUP_SIZE * ROWS_DEV
    grad_coef = 1.0 / (2 * batch_total * TEMPERATURE)

    def block_step(carry, row_blocks):
        loss_acc, proto_acc = carry
        rows_one, rows_two = row_blocks
        score_one = scores_of(rows_one, protos)
        score_two = scores_of(rows_two, protos)
        plan_one = jnp.exp(score_one / EPSILON) * scale_one
        plan_two = jnp.exp(score_two / EPSILON) * scale_two
        codes_one = plan_one / jnp.sum(plan_one, axis=1, keepdims=True)
        codes_two = plan_two / jnp.sum(plan_two, axis=1, keepdims=True)
        logp_one = jax.nn.log_softmax(score_one / TEMPERATURE, axis=1)
        logp_two = jax.nn.log_softmax(score_two / TEMPERATURE, axis=1)
        part_loss = jnp.sum(codes_two * logp_one) + jnp.sum(codes_one * logp_two)
        grad_s_one = ((jnp.exp(logp_one) - codes_two) * grad_coef).astype(jnp.bfloat16)
        grad_s_two = ((jnp.exp(logp_two) - codes_one) * grad_coef).astype(jnp.bfloat16)
        dz_one = jnp.dot(grad_s_one, protos, preferred_element_type=jnp.float32)
        dz_two = jnp.dot(grad_s_two, protos, preferred_element_type=jnp.float32)
        proto_part = jnp.dot(grad_s_one.T, rows_one, preferred_element_type=jnp.float32) + jnp.dot(grad_s_two.T, rows_two, preferred_element_type=jnp.float32)
        return (loss_acc + part_loss, proto_acc + proto_part), (codes_one, codes_two, dz_one, dz_two)

    start_carry = (jnp.zeros((), jnp.float32), jnp.zeros((PROTOS, EMBED_DIM), jnp.float32))
    (loss_sum, grad_protos), (codes_one, codes_two, dz_one, dz_two) = lax.scan(block_step, start_carry, (batch_one, batch_two))
    swap_loss = -loss_sum / (2 * batch_total)
    return (
        codes_one.reshape(batch_total, PROTOS),
        codes_two.reshape(batch_total, PROTOS),
        swap_loss,
        dz_one.reshape(batch_total, EMBED_DIM),
        dz_two.reshape(batch_total, EMBED_DIM),
        grad_protos,
    )
```

```python
import functools
import math

import jax
import jax.numpy as jnp
from jax import lax
from jax.experimental import pallas as pl
from jax.experimental.pallas import tpu as pltpu
from jax.sharding import PartitionSpec as P

EPSILON = 0.05
TEMPERATURE = 0.1
ROUNDS = 3
LANES = 128
MESH = pl.DeviceIdType.MESH
F32 = jnp.float32
BF16 = jnp.bfloat16
NT = (((1,), (1,)), ((), ()))


def kernel(
    n, protos, batch, queue,
    z1_hbm, z2_hbm, c_hbm, q1_hbm, q2_hbm,
    codes1_hbm, codes2_hbm, loss_ref, dz1_hbm, dz2_hbm, gp_hbm,
    craw, cpad, zall, qbuf, zt, atr, aall, pall, s10, lse, gbuf, gacc, wbuf, cpart, csum, lossx,
    codes, dz, gp,
    in_sem, out_sem, send_sem, recv_sem, zsend_sem, zrecv_sem, lsend_sem, lrecv_sem,
):
    tiles = cpad.shape[0] // LANES
    rows = batch + queue
    total_rows = n * rows
    batch_total = n * batch
    coef = 1.0 / (2 * batch_total * TEMPERATURE)
    scale10 = math.log2(math.e) / TEMPERATURE

    me = lax.axis_index("data")
    bit0 = lax.rem(me, 2)
    bit1 = lax.rem(me // 2, 2)
    bit2 = me // 4

    def peer(k):
        b0, b1, b2 = k % 2, (k // 2) % 2, k // 4
        return (lax.rem(bit2 + b2, 2) * 2 + lax.rem(bit1 + b1, 2)) * 2 + lax.rem(bit0 + b0, 2)

    far_first = (6, 7, 4, 5, 2, 3, 1)

    c_in = pltpu.make_async_copy(c_hbm, craw, in_sem.at[0])
    z_in = [pltpu.make_async_copy(h, zall.at[me, v], in_sem.at[1 + v]) for v, h in enumerate((z1_hbm, z2_hbm))]
    q_in = [pltpu.make_async_copy(h, qbuf.at[v], in_sem.at[3 + v]) for v, h in enumerate((q1_hbm, q2_hbm))]
    c_in.start()
    z_in[0].start()
    q_in[0].start()
    z_in[1].start()
    q_in[1].start()

    barrier = pltpu.get_barrier_semaphore()
    for k in far_first:
        pl.semaphore_signal(barrier, inc=1, device_id=(peer(k),), device_id_type=MESH)

    c_in.wait()
    cpad[pl.ds(protos // 16 * 16, cpad.shape[0] - protos // 16 * 16), :] = jnp.zeros(
        (cpad.shape[0] - protos // 16 * 16, LANES), BF16)
    cpad[pl.ds(0, protos), :] = craw[...]

    lane = lax.broadcasted_iota(jnp.int32, (1, LANES), 1)
    tail_ok = lane < (protos - (tiles - 1) * LANES)
    tail_mask = tail_ok.astype(F32)

    def fold(x):
        return jnp.sum(x.reshape(x.shape[0] // 8, 8, LANES), axis=0)

    def publish(t, v, acc):
        for j in range(tiles):
            cpart[v, pl.ds(8 * j, 8), :] = acc[j]
        out = cpart[v, pl.ds(0, tiles, stride=8), :]
        for s in range(1, 8):
            out = out + cpart[v, pl.ds(s, tiles, stride=8), :]
        csum[t, v, me] = out

    def sum_copy(t, v, k):
        return pltpu.make_async_remote_copy(
            src_ref=csum.at[t, v, me], dst_ref=csum.at[t, v, me],
            send_sem=send_sem.at[t, v, k - 1], recv_sem=recv_sem.at[t, v, k - 1],
            device_id=(peer(k),), device_id_type=MESH)

    def send_sums(t, v):
        for k in far_first:
            sum_copy(t, v, k).start()

    def col_scale(t, v):
        for k in far_first:
            sum_copy(t, v, k).wait_recv()
        c = csum[t, v, 0]
        for d in range(1, n):
            c = c + csum[t, v, d]
        w = 1.0 / (protos * c)
        index = (lax.broadcasted_iota(jnp.int32, (tiles, LANES), 0) * LANES
                 + lax.broadcasted_iota(jnp.int32, (tiles, LANES), 1))
        wbuf[v] = jnp.where(index < protos, w, 0.0)

    def first_pass(v):
        acc = [jnp.zeros((8, LANES), F32) for _ in range(tiles)]
        blocks = [(zall.at[me, v], 0, batch)]
        step = queue // 2
        blocks += [(qbuf.at[v, pl.ds(i * step, step)], batch + i * step, step) for i in range(2)]
        for ref, start, size in blocks:
            x = ref[...]
            for jj in range(tiles // 2):
                s = lax.dot_general(x, cpad[pl.ds(jj * 256, 256), :], NT, preferred_element_type=F32)
                for h in range(2):
                    e = jnp.exp2(s[:, h * LANES:(h + 1) * LANES] * scale10)
                    a = e * e
                    atr[v, 2 * jj + h, pl.ds(start, size), :] = a
                    acc[2 * jj + h] = acc[2 * jj + h] + fold(a)
        return acc

    def sink_pass(v):
        acc = [jnp.zeros((8, LANES), F32) for _ in range(tiles)]
        step = 128
        for b in range(rows // step):
            sl = pl.ds(b * step, step)
            p = atr[v, 0, sl, :] * wbuf[v, 0:1, :]
            for j in range(1, tiles):
                p = p + atr[v, j, sl, :] * wbuf[v, j:j + 1, :]
            u = 1.0 / (total_rows * jnp.sum(p, axis=1, keepdims=True))
            for j in range(tiles):
                acc[j] = acc[j] + fold(atr[v, j, sl, :] * u)
        return acc

    z_in[0].wait()
    q_in[0].wait()
    publish(0, 0, first_pass(0))
    pl.semaphore_wait(barrier, n - 1)
    send_sums(0, 0)
    z_in[1].wait()
    q_in[1].wait()
    publish(0, 1, first_pass(1))
    send_sums(0, 1)

    def z_copy(k, owner):
        return pltpu.make_async_remote_copy(
            src_ref=zall.at[owner], dst_ref=zall.at[owner],
            send_sem=zsend_sem.at[k - 1], recv_sem=zrecv_sem.at[k - 1],
            device_id=(peer(k if k in (1, 2, 4, 6) else 1),), device_id_type=MESH)

    for k in (6, 2, 4, 1):
        z_copy(k, me).start()

    def relay(k):
        z_copy(k, me).wait_recv()
        z_copy(k + 1, peer(k)).start()

    def prepare(k):
        d = peer(k)
        if k in (3, 5, 7, 1):
            z_copy(k, me).wait_recv()
        sl = pl.ds(pl.multiple_of(d * batch, batch), batch)
        x = zall[d].reshape(2 * batch, LANES)
        for v in range(2):
            zt[v, :, sl] = zall[d, v].T
        p = None
        for jj in range(tiles // 2):
            s = lax.dot_general(x, cpad[pl.ds(jj * 256, 256), :], NT, preferred_element_type=F32)
            for h in range(2):
                j = 2 * jj + h
                sj = s[:, h * LANES:(h + 1) * LANES]
                e = jnp.exp2(sj * scale10)
                if j == tiles - 1:
                    e = e * tail_mask
                a = e * e
                for v in range(2):
                    half = slice(v * batch, (v + 1) * batch)
                    aall[v, j, sl, :] = a[half]
                    pall[v, j, sl, :] = e[half]
                    if k == 0:
                        s10[v, j] = sj[half] * (1.0 / TEMPERATURE)
                p = e if p is None else p + e
        r = jnp.sum(p, axis=1, keepdims=True)
        inv = coef / r
        if k == 0:
            log_r = jnp.log(r)
            for v in range(2):
                lse[v] = jnp.broadcast_to(log_r[v * batch:(v + 1) * batch], (batch, LANES))
        for v in range(2):
            for j in range(tiles):
                pall[v, j, sl, :] = pall[v, j, sl, :] * inv[v * batch:(v + 1) * batch]

    prepare(0)
    for v in range(2):
        col_scale(0, v)
        publish(1, v, sink_pass(v))
        send_sums(1, v)

    for k in (2, 4, 6):
        relay(k)
    for k in (1, 2, 4):
        prepare(k)
    for v in range(2):
        col_scale(1, v)
        publish(2, v, sink_pass(v))
        send_sums(2, v)
    for k in (6, 3, 5, 7):
        prepare(k)

    own = pl.ds(pl.multiple_of(me * batch, batch), batch)

    def own_codes(v):
        p = None
        for j in range(tiles):
            t = aall[v, j, own, :] * wbuf[v, j:j + 1, :]
            p = t if p is None else p + t
        inv = 1.0 / jnp.sum(p, axis=1, keepdims=True)
        part = jnp.zeros((8, LANES), F32)
        for j in range(tiles):
            q = aall[v, j, own, :] * wbuf[v, j:j + 1, :] * inv
            width = min(LANES, protos - j * LANES)
            codes[v, :, j * LANES:j * LANES + width] = q[:, :width]
            part = part + fold(q * (s10[1 - v, j] - lse[1 - v]))
        return part

    def final_pass(v):
        for d in range(n):
            sl = pl.ds(d * batch, batch)
            p = None
            for j in range(tiles):
                t = aall[v, j, sl, :] * wbuf[v, j:j + 1, :]
                p = t if p is None else p + t
            q = coef / jnp.sum(p, axis=1, keepdims=True)
            for j in range(tiles):
                g = pall[1 - v, j, sl, :] - aall[v, j, sl, :] * wbuf[v, j:j + 1, :] * q
                gbuf[1 - v, j // 2, sl, (j % 2) * LANES:(j % 2 + 1) * LANES] = g.astype(BF16)

    loss_part = []
    outs = []

    def out(src, dst, i):
        copy = pltpu.make_async_copy(src, dst, out_sem.at[i])
        copy.start()
        outs.append(copy)

    def finish(v):
        col_scale(2, v)
        loss_part.append(own_codes(v))
        out(codes.at[v], (codes1_hbm, codes2_hbm)[v], v)

    def loss_copy(k):
        return pltpu.make_async_remote_copy(
            src_ref=lossx.at[me], dst_ref=lossx.at[me],
            send_sem=lsend_sem.at[k - 1], recv_sem=lrecv_sem.at[k - 1],
            device_id=(peer(k),), device_id_type=MESH)

    def dz_of(v):
        o = None
        for jj in range(tiles // 2):
            t = jnp.dot(gbuf[v, jj, own, :], cpad[pl.ds(jj * 256, 256), :], preferred_element_type=F32)
            o = t if o is None else o + t
        dz[v] = o
        out(dz.at[v], (dz1_hbm, dz2_hbm)[v], 2 + v)

    finish(0)
    final_pass(0)
    for jj in range(tiles // 2):
        gacc[jj] = jnp.dot(zt[1], gbuf[1, jj], preferred_element_type=F32)
    dz_of(1)
    finish(1)
    lossx[me] = loss_part[0] + loss_part[1]
    for k in far_first:
        loss_copy(k).start()
    final_pass(1)
    for jj in range(tiles // 2):
        g = gacc[jj] + jnp.dot(zt[0], gbuf[0, jj], preferred_element_type=F32)
        size = min(256, protos - jj * 256)
        gp[pl.ds(jj * 256, size), :] = g.T[:size]
    out(gp, gp_hbm, 4)
    dz_of(0)

    for k in far_first:
        loss_copy(k).wait_recv()
    acc = lossx[0]
    for d in range(1, n):
        acc = acc + lossx[d]
    loss_ref[0, 0] = jnp.sum(acc) * (-1.0 / (2 * batch_total))

    for t in range(ROUNDS):
        for v in range(2):
            for k in far_first:
                sum_copy(t, v, k).wait_send()
    for k in range(1, n):
        z_copy(k, me).wait_send()
        loss_copy(k).wait_send()
    for copy in outs:
        copy.wait()


def solution(mesh):
    n = mesh.shape["data"]

    def local_step(z_one, z_two, protos, queue_one, queue_two):
        k, width = protos.shape
        batch, queue = z_one.shape[0], queue_one.shape[0]
        rows = batch + queue
        pad = (k + 255) // 256 * 256
        tiles = pad // LANES
        anywhere = pl.BlockSpec(memory_space=pl.ANY)
        sem = pltpu.SemaphoreType.DMA
        outs = pl.pallas_call(
            functools.partial(kernel, n, k, batch, queue),
            out_shape=(
                jax.ShapeDtypeStruct((batch, k), F32),
                jax.ShapeDtypeStruct((batch, k), F32),
                jax.ShapeDtypeStruct((1, 1), F32),
                jax.ShapeDtypeStruct((batch, width), F32),
                jax.ShapeDtypeStruct((batch, width), F32),
                jax.ShapeDtypeStruct((k, width), F32),
            ),
            in_specs=[anywhere] * 5,
            out_specs=(anywhere, anywhere, pl.BlockSpec(memory_space=pltpu.SMEM), anywhere, anywhere, anywhere),
            scratch_shapes=[
                pltpu.VMEM((k, width), BF16),
                pltpu.VMEM((pad, width), BF16),
                pltpu.VMEM((n, 2, batch, width), BF16),
                pltpu.VMEM((2, queue, width), BF16),
                pltpu.VMEM((2, width, n * batch), BF16),
                pltpu.VMEM((2, tiles, rows, LANES), F32),
                pltpu.VMEM((2, tiles, n * batch, LANES), F32),
                pltpu.VMEM((2, tiles, n * batch, LANES), F32),
                pltpu.VMEM((2, tiles, batch, LANES), F32),
                pltpu.VMEM((2, batch, LANES), F32),
                pltpu.VMEM((2, tiles // 2, n * batch, 256), BF16),
                pltpu.VMEM((tiles // 2, width, 256), F32),
                pltpu.VMEM((2, tiles, LANES), F32),
                pltpu.VMEM((2, 8 * tiles, LANES), F32),
                pltpu.VMEM((ROUNDS, 2, n, tiles, LANES), F32),
                pltpu.VMEM((n, 8, LANES), F32),
                pltpu.VMEM((2, batch, k), F32),
                pltpu.VMEM((2, batch, width), F32),
                pltpu.VMEM((k, width), F32),
                sem((5,)),
                sem((5,)),
                sem((ROUNDS, 2, n - 1)),
                sem((ROUNDS, 2, n - 1)),
                sem((n - 1,)),
                sem((n - 1,)),
                sem((n - 1,)),
                sem((n - 1,)),
            ],
            compiler_params=pltpu.CompilerParams(collective_id=0, has_side_effects=True),
        )(z_one, z_two, protos, queue_one, queue_two)
        codes_one, codes_two, loss, dz_one, dz_two, grad_protos = outs
        return codes_one, codes_two, loss[0, 0], dz_one, dz_two, grad_protos

    row_spec = P("data", None)
    full_spec = P(None, None)
    return jax.shard_map(
        local_step,
        mesh=mesh,
        in_specs=(row_spec, row_spec, full_spec, row_spec, row_spec),
        out_specs=(row_spec, row_spec, P(), row_spec, row_spec, full_spec),
        check_vma=False,
    )
```

```python
import functools
import math

import jax
import jax.numpy as jnp
from jax import lax
from jax.experimental import pallas as pl
from jax.experimental.pallas import tpu as pltpu
from jax.sharding import PartitionSpec as P

EPSILON = 0.05
TEMPERATURE = 0.1
ROUNDS = 3
LANES = 128
MESH = pl.DeviceIdType.MESH
F32 = jnp.float32
BF16 = jnp.bfloat16
NT = (((1,), (1,)), ((), ()))


def sums_kernel(
    n, protos, batch, queue,
    z1_hbm, z2_hbm, c_hbm, q1_hbm, q2_hbm,
    aall, pall, sall, zt, cpad, wbuf, lse_sum,
    craw, zall, qbuf, atr, cpart, csum,
    in_sem, send_sem, recv_sem, zsend_sem, zrecv_sem,
):
    tiles = cpad.shape[0] // LANES
    rows = batch + queue
    total_rows = n * rows
    coef = 1.0 / (2 * n * batch * TEMPERATURE)
    scale10 = math.log2(math.e) / TEMPERATURE

    me = lax.axis_index("data")
    bit0 = lax.rem(me, 2)
    bit1 = lax.rem(me // 2, 2)
    bit2 = me // 4

    def peer(k):
        b0, b1, b2 = k % 2, (k // 2) % 2, k // 4
        return (lax.rem(bit2 + b2, 2) * 2 + lax.rem(bit1 + b1, 2)) * 2 + lax.rem(bit0 + b0, 2)

    far_first = (6, 7, 4, 5, 2, 3, 1)

    c_in = pltpu.make_async_copy(c_hbm, craw, in_sem.at[0])
    z_in = [pltpu.make_async_copy(h, zall.at[me, v], in_sem.at[1 + v]) for v, h in enumerate((z1_hbm, z2_hbm))]
    q_in = [pltpu.make_async_copy(h, qbuf.at[v], in_sem.at[3 + v]) for v, h in enumerate((q1_hbm, q2_hbm))]
    c_in.start()
    z_in[0].start()
    q_in[0].start()
    z_in[1].start()
    q_in[1].start()

    barrier = pltpu.get_barrier_semaphore()
    for k in far_first:
        pl.semaphore_signal(barrier, inc=1, device_id=(peer(k),), device_id_type=MESH)

    c_in.wait()
    cpad[pl.ds(protos // 16 * 16, cpad.shape[0] - protos // 16 * 16), :] = jnp.zeros(
        (cpad.shape[0] - protos // 16 * 16, LANES), BF16)
    cpad[pl.ds(0, protos), :] = craw[...]

    lane = lax.broadcasted_iota(jnp.int32, (1, LANES), 1)
    tail_ok = lane < (protos - (tiles - 1) * LANES)
    tail_mask = tail_ok.astype(F32)

    def fold(x):
        return jnp.sum(x.reshape(x.shape[0] // 8, 8, LANES), axis=0)

    def publish(t, v, acc):
        for j in range(tiles):
            cpart[v, pl.ds(8 * j, 8), :] = acc[j]
        out = cpart[v, pl.ds(0, tiles, stride=8), :]
        for s in range(1, 8):
            out = out + cpart[v, pl.ds(s, tiles, stride=8), :]
        csum[t, v, me] = out

    def sum_copy(t, v, k):
        return pltpu.make_async_remote_copy(
            src_ref=csum.at[t, v, me], dst_ref=csum.at[t, v, me],
            send_sem=send_sem.at[t, v, k - 1], recv_sem=recv_sem.at[t, v, k - 1],
            device_id=(peer(k),), device_id_type=MESH)

    def send_sums(t, v):
        for k in far_first:
            sum_copy(t, v, k).start()

    def col_scale(t, v):
        for k in far_first:
            sum_copy(t, v, k).wait_recv()
        c = csum[t, v, 0]
        for d in range(1, n):
            c = c + csum[t, v, d]
        w = 1.0 / (protos * c)
        index = (lax.broadcasted_iota(jnp.int32, (tiles, LANES), 0) * LANES
                 + lax.broadcasted_iota(jnp.int32, (tiles, LANES), 1))
        wbuf[v] = jnp.where(index < protos, w, 0.0)

    def first_pass(v):
        acc = [jnp.zeros((8, LANES), F32) for _ in range(tiles)]
        blocks = [(zall.at[me, v], 0, batch)]
        step = queue // 2
        blocks += [(qbuf.at[v, pl.ds(i * step, step)], batch + i * step, step) for i in range(2)]
        for ref, start, size in blocks:
            x = ref[...]
            for jj in range(tiles // 2):
                s = lax.dot_general(x, cpad[pl.ds(jj * 256, 256), :], NT, preferred_element_type=F32)
                for h in range(2):
                    e = jnp.exp2(s[:, h * LANES:(h + 1) * LANES] * scale10)
                    a = e * e
                    atr[v, 2 * jj + h, pl.ds(start, size), :] = a
                    acc[2 * jj + h] = acc[2 * jj + h] + fold(a)
        return acc

    def sink_pass(v):
        acc = [jnp.zeros((8, LANES), F32) for _ in range(tiles)]
        step = 128
        for b in range(rows // step):
            sl = pl.ds(b * step, step)
            p = atr[v, 0, sl, :] * wbuf[v, 0:1, :]
            for j in range(1, tiles):
                p = p + atr[v, j, sl, :] * wbuf[v, j:j + 1, :]
            u = 1.0 / (total_rows * jnp.sum(p, axis=1, keepdims=True))
            for j in range(tiles):
                acc[j] = acc[j] + fold(atr[v, j, sl, :] * u)
        return acc

    z_in[0].wait()
    q_in[0].wait()
    publish(0, 0, first_pass(0))
    pl.semaphore_wait(barrier, n - 1)
    send_sums(0, 0)
    z_in[1].wait()
    q_in[1].wait()
    publish(0, 1, first_pass(1))
    send_sums(0, 1)

    def z_copy(k, owner):
        return pltpu.make_async_remote_copy(
            src_ref=zall.at[owner], dst_ref=zall.at[owner],
            send_sem=zsend_sem.at[k - 1], recv_sem=zrecv_sem.at[k - 1],
            device_id=(peer(k if k in (1, 2, 4, 6) else 1),), device_id_type=MESH)

    for k in (6, 2, 4, 1):
        z_copy(k, me).start()

    def relay(k):
        z_copy(k, me).wait_recv()
        z_copy(k + 1, peer(k)).start()

    def prepare(k):
        d = peer(k)
        if k in (3, 5, 7, 1):
            z_copy(k, me).wait_recv()
        sl = pl.ds(pl.multiple_of(d * batch, batch), batch)
        x = zall[d].reshape(2 * batch, LANES)
        for v in range(2):
            zt[v, :, sl] = zall[d, v].T
        p = None
        for jj in range(tiles // 2):
            s = lax.dot_general(x, cpad[pl.ds(jj * 256, 256), :], NT, preferred_element_type=F32)
            for h in range(2):
                j = 2 * jj + h
                sj = s[:, h * LANES:(h + 1) * LANES]
                e = jnp.exp2(sj * scale10)
                if j == tiles - 1:
                    e = e * tail_mask
                a = e * e
                for v in range(2):
                    half = slice(v * batch, (v + 1) * batch)
                    aall[v, j, sl, :] = a[half]
                    pall[v, j, sl, :] = e[half]
                    sall[v, j, sl, :] = sj[half]
                p = e if p is None else p + e
        r = jnp.sum(p, axis=1, keepdims=True)
        inv = coef / r
        lse_sum[d] = fold(jnp.broadcast_to(jnp.log(r), (2 * batch, LANES)))
        for v in range(2):
            for j in range(tiles):
                pall[v, j, sl, :] = pall[v, j, sl, :] * inv[v * batch:(v + 1) * batch]

    prepare(0)
    for v in range(2):
        col_scale(0, v)
        publish(1, v, sink_pass(v))
        send_sums(1, v)

    for k in (2, 4, 6):
        relay(k)
    for k in (1, 2, 4):
        prepare(k)
    for v in range(2):
        col_scale(1, v)
        publish(2, v, sink_pass(v))
        send_sums(2, v)
    for k in (6, 3, 5, 7):
        prepare(k)

    for v in range(2):
        col_scale(2, v)
    for t in range(ROUNDS):
        for v in range(2):
            for k in far_first:
                sum_copy(t, v, k).wait_send()
    for k in range(1, n):
        z_copy(k, me).wait_send()


def grads_kernel(
    n, protos, batch,
    aall, pall, sall, zt, cpad, wbuf, lse_sum,
    codes1_hbm, codes2_hbm, loss_ref, dz1_hbm, dz2_hbm, gp_hbm,
    gbuf, gacc, codes, dz, gp, out_sem,
):
    tiles = cpad.shape[0] // LANES
    batch_total = n * batch
    coef = 1.0 / (2 * batch_total * TEMPERATURE)
    me = lax.axis_index("data")
    own = pl.ds(pl.multiple_of(me * batch, batch), batch)

    def fold(x):
        return jnp.sum(x.reshape(x.shape[0] // 8, 8, LANES), axis=0)

    def own_codes(v):
        p = None
        for j in range(tiles):
            t = aall[v, j, own, :] * wbuf[v, j:j + 1, :]
            p = t if p is None else p + t
        inv = 1.0 / jnp.sum(p, axis=1, keepdims=True)
        for j in range(tiles):
            q = aall[v, j, own, :] * wbuf[v, j:j + 1, :] * inv
            size = min(LANES, protos - j * LANES)
            codes[v, pl.ds(j * LANES, size), :] = q.T[:size]

    def final_pass(v):
        part = jnp.zeros((8, LANES), F32)
        for d in range(n):
            sl = pl.ds(d * batch, batch)
            p = None
            m = None
            for j in range(tiles):
                t = aall[v, j, sl, :] * wbuf[v, j:j + 1, :]
                u = t * sall[1 - v, j, sl, :]
                p = t if p is None else p + t
                m = u if m is None else m + u
            q = coef / jnp.sum(p, axis=1, keepdims=True)
            part = part + fold(m * q)
            for j in range(tiles):
                g = pall[1 - v, j, sl, :] - aall[v, j, sl, :] * wbuf[v, j:j + 1, :] * q
                gbuf[1 - v, j // 2, sl, (j % 2) * LANES:(j % 2 + 1) * LANES] = g.astype(BF16)
        return part

    outs = []

    def out(src, dst):
        copy = pltpu.make_async_copy(src, dst, out_sem.at[len(outs)])
        copy.start()
        outs.append(copy)

    def dz_of(v):
        o = None
        for jj in range(tiles // 2):
            t = jnp.dot(gbuf[v, jj, own, :], cpad[pl.ds(jj * 256, 256), :], preferred_element_type=F32)
            o = t if o is None else o + t
        dz[v] = o
        out(dz.at[v], (dz1_hbm, dz2_hbm)[v])

    own_codes(0)
    out(codes.at[0], codes1_hbm)
    own_codes(1)
    out(codes.at[1], codes2_hbm)
    part = final_pass(0)
    for jj in range(tiles // 2):
        gacc[jj] = jnp.dot(zt[1], gbuf[1, jj], preferred_element_type=F32)
    dz_of(1)
    part = part + final_pass(1)
    for jj in range(tiles // 2):
        g = gacc[jj] + jnp.dot(zt[0], gbuf[0, jj], preferred_element_type=F32)
        size = min(256, protos - jj * 256)
        gp[pl.ds(jj * 256, size), :] = g.T[:size]
    out(gp, gp_hbm)
    dz_of(0)

    logs = lse_sum[0]
    for d in range(1, n):
        logs = logs + lse_sum[d]
    scaled = jnp.sum(part) / (coef * TEMPERATURE) - jnp.sum(logs) / LANES
    loss_ref[0, 0] = scaled * (-1.0 / (2 * batch_total))
    for copy in outs:
        copy.wait()


def solution(mesh):
    n = mesh.shape["data"]

    def local_step(z_one, z_two, protos, queue_one, queue_two):
        k, width = protos.shape
        batch, queue = z_one.shape[0], queue_one.shape[0]
        rows = batch + queue
        pad = (k + 255) // 256 * 256
        tiles = pad // LANES
        anywhere = pl.BlockSpec(memory_space=pl.ANY)
        sem = pltpu.SemaphoreType.DMA
        vmem = pl.BlockSpec(memory_space=pltpu.VMEM)
        whole = n * batch
        shared = pl.pallas_call(
            functools.partial(sums_kernel, n, k, batch, queue),
            out_shape=(
                pltpu.VMEM((2, tiles, whole, LANES), F32),
                pltpu.VMEM((2, tiles, whole, LANES), F32),
                pltpu.VMEM((2, tiles, whole, LANES), F32),
                pltpu.VMEM((2, width, whole), BF16),
                pltpu.VMEM((pad, width), BF16),
                pltpu.VMEM((2, tiles, LANES), F32),
                pltpu.VMEM((n, 8, LANES), F32),
            ),
            in_specs=[pl.BlockSpec(memory_space=pltpu.HBM)] * 5,
            out_specs=(vmem,) * 7,
            scratch_shapes=[
                pltpu.VMEM((k, width), BF16),
                pltpu.VMEM((n, 2, batch, width), BF16),
                pltpu.VMEM((2, queue, width), BF16),
                pltpu.VMEM((2, tiles, rows, LANES), F32),
                pltpu.VMEM((2, 8 * tiles, LANES), F32),
                pltpu.VMEM((ROUNDS, 2, n, tiles, LANES), F32),
                sem((5,)),
                sem((ROUNDS, 2, n - 1)),
                sem((ROUNDS, 2, n - 1)),
                sem((n - 1,)),
                sem((n - 1,)),
            ],
            compiler_params=pltpu.CompilerParams(
                collective_id=0, has_side_effects=True, vmem_limit_bytes=14 << 20),
            name="sums",
        )(*(pltpu.with_memory_space_constraint(x, pltpu.HBM) for x in (z_one, z_two, protos, queue_one, queue_two)))
        codes_one, codes_two, loss, dz_one, dz_two, grad_protos = pl.pallas_call(
            functools.partial(grads_kernel, n, k, batch),
            out_shape=(
                jax.ShapeDtypeStruct((k, batch), F32),
                jax.ShapeDtypeStruct((k, batch), F32),
                jax.ShapeDtypeStruct((1, 1), F32),
                jax.ShapeDtypeStruct((batch, width), F32),
                jax.ShapeDtypeStruct((batch, width), F32),
                jax.ShapeDtypeStruct((k, width), F32),
            ),
            in_specs=[vmem] * 7,
            out_specs=(anywhere, anywhere, pl.BlockSpec(memory_space=pltpu.SMEM), anywhere, anywhere, anywhere),
            scratch_shapes=[
                pltpu.VMEM((2, tiles // 2, whole, 256), BF16),
                pltpu.VMEM((tiles // 2, width, 256), F32),
                pltpu.VMEM((2, k, batch), F32),
                pltpu.VMEM((2, batch, width), F32),
                pltpu.VMEM((k, width), F32),
                sem((5,)),
            ],
            compiler_params=pltpu.CompilerParams(vmem_limit_bytes=14 << 20),
            name="grads",
        )(*shared)
        return codes_one.T, codes_two.T, loss[0, 0], dz_one, dz_two, grad_protos

    row_spec = P("data", None)
    full_spec = P(None, None)
    return jax.shard_map(
        local_step,
        mesh=mesh,
        in_specs=(row_spec, row_spec, full_spec, row_spec, row_spec),
        out_specs=(row_spec, row_spec, P(), row_spec, row_spec, full_spec),
        check_vma=False,
    )
```

```python
import functools
import math

import jax
import jax.numpy as jnp
from jax import lax
from jax.experimental import pallas as pl
from jax.experimental.pallas import tpu as pltpu
from jax.sharding import PartitionSpec as P

EPSILON = 0.05
TEMPERATURE = 0.1
ROUNDS = 3
LANES = 128
MESH = pl.DeviceIdType.MESH
F32 = jnp.float32
BF16 = jnp.bfloat16
NT = (((1,), (1,)), ((), ()))


def fold(x):
    return jnp.sum(x.reshape(x.shape[0] // 8, 8, LANES), axis=0)


def sums_kernel(
    n, protos, batch, queue,
    z1_hbm, z2_hbm, c_hbm, q1_hbm, q2_hbm,
    aall, pall, rinv, zt, cpad, wbuf, loss_part, lse_sum,
    xbuf, zall, sall, atr, cpart, csum,
    in_sem, send_sem, recv_sem, zsend_sem, zrecv_sem,
):
    tiles = cpad.shape[0] // LANES
    rows = batch + queue
    total_rows = n * rows
    coef = 1.0 / (2 * n * batch * TEMPERATURE)
    scale10 = math.log2(math.e) / TEMPERATURE

    me = lax.axis_index("data")
    bit0 = lax.rem(me, 2)
    bit1 = lax.rem(me // 2, 2)
    bit2 = me // 4

    def peer(k):
        b0, b1, b2 = k % 2, (k // 2) % 2, k // 4
        return (lax.rem(bit2 + b2, 2) * 2 + lax.rem(bit1 + b1, 2)) * 2 + lax.rem(bit0 + b0, 2)

    far_first = (6, 7, 4, 5, 2, 3, 1)

    c_in = pltpu.make_async_copy(c_hbm, cpad.at[pl.ds(0, protos)], in_sem.at[2])

    def rows_in(v):
        z_hbm, q_hbm = ((z1_hbm, q1_hbm), (z2_hbm, q2_hbm))[v]
        pltpu.make_async_copy(z_hbm, xbuf.at[v, pl.ds(0, batch)], in_sem.at[v]).start()
        pltpu.make_async_copy(q_hbm, xbuf.at[v, pl.ds(batch, queue)], in_sem.at[v]).start()

    def wait_rows(v):
        pltpu.make_async_copy(xbuf.at[v], xbuf.at[v], in_sem.at[v]).wait()

    c_in.start()
    rows_in(0)
    rows_in(1)

    barrier = pltpu.get_barrier_semaphore()
    for k in far_first:
        pl.semaphore_signal(barrier, inc=1, device_id=(peer(k),), device_id_type=MESH)

    cpad[pl.ds(protos, cpad.shape[0] - protos), :] = jnp.zeros((cpad.shape[0] - protos, LANES), BF16)
    c_in.wait()

    lane = lax.broadcasted_iota(jnp.int32, (1, LANES), 1)
    tail_ok = lane < (protos - (tiles - 1) * LANES)
    tail_mask = tail_ok.astype(F32)

    def publish(t, v, acc):
        for j in range(tiles):
            cpart[v, pl.ds(8 * j, 8), :] = acc[j]
        out = cpart[v, pl.ds(0, tiles, stride=8), :]
        for s in range(1, 8):
            out = out + cpart[v, pl.ds(s, tiles, stride=8), :]
        csum[t, v, me] = out

    def sum_copy(t, v, k, slots):
        return pltpu.make_async_remote_copy(
            src_ref=csum.at[t, v, slots], dst_ref=csum.at[t, v, slots],
            send_sem=send_sem.at[v], recv_sem=recv_sem.at[t, v],
            device_id=(peer(k),), device_id_type=MESH)

    def all_sums(t, v):
        return sum_copy(t, v, 1, pl.ds(0, n - 1))

    def send_sums(t, v):
        if t > 0:
            all_sums(t, v).wait_send()
        for k in far_first:
            sum_copy(t, v, k, me).start()

    def col_scale(t, v):
        all_sums(t, v).wait_recv()
        c = csum[t, v, 0]
        for d in range(1, n):
            c = c + csum[t, v, d]
        w = 1.0 / (protos * c)
        index = (lax.broadcasted_iota(jnp.int32, (tiles, LANES), 0) * LANES
                 + lax.broadcasted_iota(jnp.int32, (tiles, LANES), 1))
        wbuf[v] = jnp.where(index < protos, w, 0.0)

    def first_pass(v):
        acc = [jnp.zeros((8, LANES), F32) for _ in range(tiles)]
        for start, size in ((0, rows // 2), (rows // 2, rows // 2)):
            x = xbuf[v, pl.ds(start, size), :]
            for jj in range(tiles // 2):
                s = lax.dot_general(x, cpad[pl.ds(jj * 256, 256), :], NT, preferred_element_type=F32)
                for h in range(2):
                    e = jnp.exp2(s[:, h * LANES:(h + 1) * LANES] * scale10)
                    a = e * e
                    atr[v, 2 * jj + h, pl.ds(start, size), :] = a
                    acc[2 * jj + h] = acc[2 * jj + h] + fold(a)
        return acc

    def sink_pass(v):
        acc = [jnp.zeros((8, LANES), F32) for _ in range(tiles)]
        step = 128
        for b in range(rows // step):
            sl = pl.ds(b * step, step)
            p = atr[v, 0, sl, :] * wbuf[v, 0:1, :]
            for j in range(1, tiles):
                p = p + atr[v, j, sl, :] * wbuf[v, j:j + 1, :]
            u = 1.0 / (total_rows * jnp.sum(p, axis=1, keepdims=True))
            for j in range(tiles):
                acc[j] = acc[j] + fold(atr[v, j, sl, :] * u)
        return acc

    wait_rows(0)
    publish(0, 0, first_pass(0))
    pl.semaphore_wait(barrier, n - 1)
    send_sums(0, 0)
    wait_rows(1)
    publish(0, 1, first_pass(1))
    send_sums(0, 1)

    def z_copy(k, target, src, dst):
        return pltpu.make_async_remote_copy(
            src_ref=src, dst_ref=dst, send_sem=zsend_sem.at[0], recv_sem=zrecv_sem.at[k - 1],
            device_id=(peer(target),), device_id_type=MESH)

    for k in (6, 2, 4, 1):
        for v in range(2):
            z_copy(k, k, xbuf.at[v, pl.ds(0, batch)], zall.at[me, v]).start()

    def z_arrived(k):
        z_copy(k, k, zall.at[peer(k)], zall.at[peer(k)]).wait_recv()

    def relay(k):
        z_arrived(k)
        z_copy(k + 1, 1, zall.at[peer(k)], zall.at[peer(k)]).start()

    def prepare(k):
        d = peer(k)
        if k in (3, 5, 7, 1):
            z_arrived(k)
        sl = pl.ds(pl.multiple_of(d * batch, batch), batch)
        z = [xbuf[v, pl.ds(0, batch), :] if k == 0 else zall[d, v] for v in range(2)]
        for v in range(2):
            zt[:, pl.ds(pl.multiple_of((v * n + d) * batch, batch), batch)] = z[v].T
        x = jnp.concatenate(z, axis=0)
        p = None
        for jj in range(tiles // 2):
            s = lax.dot_general(x, cpad[pl.ds(jj * 256, 256), :], NT, preferred_element_type=F32)
            for h in range(2):
                j = 2 * jj + h
                sj = s[:, h * LANES:(h + 1) * LANES]
                e = jnp.exp2(sj * scale10)
                if j == tiles - 1:
                    e = e * tail_mask
                a = e * e
                for v in range(2):
                    half = slice(v * batch, (v + 1) * batch)
                    aall[v, j, sl, :] = a[half]
                    pall[v, j, sl, :] = e[half]
                    sall[v, j, sl, :] = sj[half]
                p = e if p is None else p + e
        r = jnp.sum(p, axis=1, keepdims=True)
        inv = coef / r
        lse_sum[d] = fold(jnp.broadcast_to(jnp.log(r), (2 * batch, LANES)))
        for v in range(2):
            for j in range(tiles):
                pall[v, j, sl, :] = pall[v, j, sl, :] * inv[v * batch:(v + 1) * batch]

    prepare(0)
    for v in range(2):
        col_scale(0, v)
        publish(1, v, sink_pass(v))
        send_sums(1, v)

    prepare(1)
    for k in (2, 4, 6):
        relay(k)
    for k in (2, 4):
        prepare(k)
    for v in range(2):
        col_scale(1, v)
        publish(2, v, sink_pass(v))
        send_sums(2, v)
    for k in (6, 3, 5, 7):
        prepare(k)


    def row_scale(v):
        part = jnp.zeros((8, LANES), F32)
        for d in range(n):
            sl = pl.ds(d * batch, batch)
            p = None
            m = None
            for j in range(tiles):
                t = aall[v, j, sl, :] * wbuf[v, j:j + 1, :]
                u = t * sall[1 - v, j, sl, :]
                p = t if p is None else p + t
                m = u if m is None else m + u
            inv = 1.0 / jnp.sum(p, axis=1, keepdims=True)
            part = part + fold(m * inv)
            rinv[v, sl, :] = jnp.broadcast_to(inv, (batch, LANES))
        return part

    col_scale(2, 0)
    part = row_scale(0)
    col_scale(2, 1)
    loss_part[...] = part + row_scale(1)

    for v in range(2):
        all_sums(2, v).wait_send()
    z_copy(1, 1, zall.at[pl.ds(0, n - 1)], zall.at[pl.ds(0, n - 1)]).wait_send()


def grads_kernel(
    n, protos, batch,
    aall, pall, rinv, zt, cpad, wbuf, loss_part, lse_sum,
    codes1_hbm, codes2_hbm, loss_ref, dz1_hbm, dz2_hbm, gp_hbm,
    gbuf, codes, dz, gp, out_sem,
):
    tiles = cpad.shape[0] // LANES
    batch_total = n * batch
    coef = 1.0 / (2 * batch_total * TEMPERATURE)
    me = lax.axis_index("data")
    own = pl.ds(pl.multiple_of(me * batch, batch), batch)
    codes_hbm = (codes1_hbm, codes2_hbm)
    dz_hbm = (dz1_hbm, dz2_hbm)

    for jj in range(tiles // 2):
        size = min(2 * LANES, protos - jj * 2 * LANES)
        cols = pl.ds(jj * 2 * LANES, size)
        for v in range(2):
            for h in range(2):
                j = 2 * jj + h
                w = wbuf[v, j:j + 1, :] * coef
                for d in range(n):
                    sl = pl.ds(d * batch, batch)
                    g = pall[1 - v, j, sl, :] - aall[v, j, sl, :] * w * rinv[v, sl, :]
                    gbuf[jj, pl.ds(((1 - v) * n + d) * batch, batch), h * LANES:(h + 1) * LANES] = g.astype(BF16)
                part = min(LANES, protos - j * LANES)
                q = aall[v, j, own, :] * wbuf[v, j:j + 1, :] * rinv[v, own, :]
                codes[v, pl.ds(j * LANES, part), :] = q.T[:part]
            pltpu.make_async_copy(codes.at[v, cols], codes_hbm[v].at[cols], out_sem.at[v]).start()
        g = jnp.dot(zt[...], gbuf[jj], preferred_element_type=F32)
        gp[cols, :] = g.T[:size]
        pltpu.make_async_copy(gp.at[cols], gp_hbm.at[cols], out_sem.at[4]).start()
        for v in range(2):
            rows = pl.ds(pl.multiple_of((v * n + me) * batch, batch), batch)
            o = jnp.dot(gbuf[jj, rows, :], cpad[pl.ds(jj * 2 * LANES, 2 * LANES), :], preferred_element_type=F32)
            dz[v] = o if jj == 0 else dz[v] + o
    for v in range(2):
        pltpu.make_async_copy(dz.at[v], dz_hbm[v], out_sem.at[2 + v]).start()

    logs = lse_sum[0]
    for d in range(1, n):
        logs = logs + lse_sum[d]
    total = jnp.sum(loss_part[...]) * (1.0 / TEMPERATURE) - jnp.sum(logs) * (1.0 / LANES)
    loss_ref[0, 0] = total * (-1.0 / (2 * batch_total))

    for v in range(2):
        pltpu.make_async_copy(codes.at[v], codes_hbm[v], out_sem.at[v]).wait()
        pltpu.make_async_copy(dz.at[v], dz_hbm[v], out_sem.at[2 + v]).wait()
    pltpu.make_async_copy(gp, gp_hbm, out_sem.at[4]).wait()


def solution(mesh):
    n = mesh.shape["data"]

    def local_step(z_one, z_two, protos, queue_one, queue_two):
        k, width = protos.shape
        batch, queue = z_one.shape[0], queue_one.shape[0]
        rows = batch + queue
        pad = (k + 255) // 256 * 256
        tiles = pad // LANES
        anywhere = pl.BlockSpec(memory_space=pl.ANY)
        sem = pltpu.SemaphoreType.DMA
        vmem = pl.BlockSpec(memory_space=pltpu.VMEM)
        whole = n * batch
        shared = pl.pallas_call(
            functools.partial(sums_kernel, n, k, batch, queue),
            out_shape=(
                pltpu.VMEM((2, tiles, whole, LANES), F32),
                pltpu.VMEM((2, tiles, whole, LANES), F32),
                pltpu.VMEM((2, whole, LANES), F32),
                pltpu.VMEM((width, 2 * whole), BF16),
                pltpu.VMEM((pad, width), BF16),
                pltpu.VMEM((2, tiles, LANES), F32),
                pltpu.VMEM((8, LANES), F32),
                pltpu.VMEM((n, 8, LANES), F32),
            ),
            in_specs=[anywhere] * 5,
            out_specs=(vmem,) * 8,
            scratch_shapes=[
                pltpu.VMEM((2, rows, width), BF16),
                pltpu.VMEM((n, 2, batch, width), BF16),
                pltpu.VMEM((2, tiles, whole, LANES), F32),
                pltpu.VMEM((2, tiles, rows, LANES), F32),
                pltpu.VMEM((2, 8 * tiles, LANES), F32),
                pltpu.VMEM((ROUNDS, 2, n, tiles, LANES), F32),
                sem((3,)),
                sem((2,)),
                sem((ROUNDS, 2)),
                sem((1,)),
                sem((n - 1,)),
            ],
            compiler_params=pltpu.CompilerParams(
                collective_id=0, has_side_effects=True, vmem_limit_bytes=20 << 20),
            name="sums",
        )(*(pltpu.with_memory_space_constraint(x, pltpu.HBM) for x in (z_one, z_two, protos, queue_one, queue_two)))
        codes_one, codes_two, loss, dz_one, dz_two, grad_protos = pl.pallas_call(
            functools.partial(grads_kernel, n, k, batch),
            out_shape=(
                jax.ShapeDtypeStruct((k, batch), F32),
                jax.ShapeDtypeStruct((k, batch), F32),
                jax.ShapeDtypeStruct((1, 1), F32),
                jax.ShapeDtypeStruct((batch, width), F32),
                jax.ShapeDtypeStruct((batch, width), F32),
                jax.ShapeDtypeStruct((k, width), F32),
            ),
            in_specs=[vmem] * 8,
            out_specs=(anywhere, anywhere, pl.BlockSpec(memory_space=pltpu.SMEM), anywhere, anywhere, anywhere),
            scratch_shapes=[
                pltpu.VMEM((tiles // 2, 2 * whole, 2 * LANES), BF16),
                pltpu.VMEM((2, k, batch), F32),
                pltpu.VMEM((2, batch, width), F32),
                pltpu.VMEM((k, width), F32),
                sem((5,)),
            ],
            compiler_params=pltpu.CompilerParams(vmem_limit_bytes=14 << 20),
            name="grads",
        )(*shared)
        return codes_one.T, codes_two.T, loss[0, 0], dz_one, dz_two, grad_protos

    row_spec = P("data", None)
    full_spec = P(None, None)
    return jax.shard_map(
        local_step,
        mesh=mesh,
        in_specs=(row_spec, row_spec, full_spec, row_spec, row_spec),
        out_specs=(row_spec, row_spec, P(), row_spec, row_spec, full_spec),
        check_vma=False,
    )
```

```python
import functools
import math

import jax
import jax.numpy as jnp
from jax import lax
from jax.experimental import pallas as pl
from jax.experimental.pallas import tpu as pltpu
from jax.sharding import PartitionSpec as P

EPSILON = 0.05
TEMPERATURE = 0.1
ROUNDS = 3
LANES = 128
MESH = pl.DeviceIdType.MESH
F32 = jnp.float32
BF16 = jnp.bfloat16
NT = (((1,), (1,)), ((), ()))


def fold(x):
    return jnp.sum(x.reshape(x.shape[0] // 8, 8, LANES), axis=0)


def sums_kernel(
    n, protos, batch, queue,
    z1_hbm, z2_hbm, c_hbm, q1_hbm, q2_hbm,
    aall, pall, rinv, zt, cpad, small, lse_sum,
    xbuf, zall, sall, atr, cpart, csum,
    in_sem, send_sem, recv_sem, zsend_sem, zrecv_sem,
):
    tiles = cpad.shape[0] // LANES
    rows = batch + queue
    total_rows = n * rows
    coef = 1.0 / (2 * n * batch * TEMPERATURE)
    scale10 = math.log2(math.e) / TEMPERATURE

    me = lax.axis_index("data")
    bit0 = lax.rem(me, 2)
    bit1 = lax.rem(me // 2, 2)
    bit2 = me // 4

    def peer(k):
        b0, b1, b2 = k % 2, (k // 2) % 2, k // 4
        return (lax.rem(bit2 + b2, 2) * 2 + lax.rem(bit1 + b1, 2)) * 2 + lax.rem(bit0 + b0, 2)

    far_first = (6, 7, 4, 5, 2, 3, 1)

    c_in = pltpu.make_async_copy(c_hbm, cpad.at[pl.ds(0, protos)], in_sem.at[2])

    def rows_in(v):
        z_hbm, q_hbm = ((z1_hbm, q1_hbm), (z2_hbm, q2_hbm))[v]
        pltpu.make_async_copy(z_hbm, xbuf.at[v, pl.ds(0, batch)], in_sem.at[v]).start()
        pltpu.make_async_copy(q_hbm, xbuf.at[v, pl.ds(batch, queue)], in_sem.at[v]).start()

    def wait_rows(v):
        pltpu.make_async_copy(xbuf.at[v], xbuf.at[v], in_sem.at[v]).wait()

    c_in.start()
    rows_in(0)
    rows_in(1)

    barrier = pltpu.get_barrier_semaphore()
    for k in far_first:
        pl.semaphore_signal(barrier, inc=1, device_id=(peer(k),), device_id_type=MESH)

    cpad[pl.ds(protos, cpad.shape[0] - protos), :] = jnp.zeros((cpad.shape[0] - protos, LANES), BF16)
    c_in.wait()

    lane = lax.broadcasted_iota(jnp.int32, (1, LANES), 1)
    tail_ok = lane < (protos - (tiles - 1) * LANES)
    tail_mask = tail_ok.astype(F32)

    def publish(t, v, acc):
        for j in range(tiles):
            cpart[v, pl.ds(8 * j, 8), :] = acc[j]
        out = cpart[v, pl.ds(0, tiles, stride=8), :]
        for s in range(1, 8):
            out = out + cpart[v, pl.ds(s, tiles, stride=8), :]
        csum[t, v, me] = out

    def sum_copy(t, v, k, slots):
        return pltpu.make_async_remote_copy(
            src_ref=csum.at[t, v, slots], dst_ref=csum.at[t, v, slots],
            send_sem=send_sem.at[v], recv_sem=recv_sem.at[t, v],
            device_id=(peer(k),), device_id_type=MESH)

    def all_sums(t, v):
        return sum_copy(t, v, 1, pl.ds(0, n - 1))

    def send_sums(t, v):
        if t > 0:
            all_sums(t, v).wait_send()
        for k in far_first:
            sum_copy(t, v, k, me).start()

    def col_scale(t, v):
        all_sums(t, v).wait_recv()
        c = csum[t, v, 0]
        for d in range(1, n):
            c = c + csum[t, v, d]
        w = 1.0 / (protos * c)
        index = (lax.broadcasted_iota(jnp.int32, (tiles, LANES), 0) * LANES
                 + lax.broadcasted_iota(jnp.int32, (tiles, LANES), 1))
        small[v] = jnp.where(index < protos, w, 0.0)

    def first_pass(v):
        acc = [jnp.zeros((8, LANES), F32) for _ in range(tiles)]
        for start, size in ((0, rows // 2), (rows // 2, rows // 2)):
            x = xbuf[v, pl.ds(start, size), :]
            for jj in range(tiles // 2):
                s = lax.dot_general(x, cpad[pl.ds(jj * 256, 256), :], NT, preferred_element_type=F32)
                for h in range(2):
                    e = jnp.exp2(s[:, h * LANES:(h + 1) * LANES] * scale10)
                    a = e * e
                    atr[v, 2 * jj + h, pl.ds(start, size), :] = a
                    acc[2 * jj + h] = acc[2 * jj + h] + fold(a)
        return acc

    def sink_pass(v):
        acc = [jnp.zeros((8, LANES), F32) for _ in range(tiles)]
        step = 128
        for b in range(rows // step):
            sl = pl.ds(b * step, step)
            p = atr[v, 0, sl, :] * small[v, 0:1, :]
            for j in range(1, tiles):
                p = p + atr[v, j, sl, :] * small[v, j:j + 1, :]
            u = 1.0 / (total_rows * jnp.sum(p, axis=1, keepdims=True))
            for j in range(tiles):
                acc[j] = acc[j] + fold(atr[v, j, sl, :] * u)
        return acc

    wait_rows(0)
    publish(0, 0, first_pass(0))
    pl.semaphore_wait(barrier, n - 1)
    send_sums(0, 0)
    wait_rows(1)
    publish(0, 1, first_pass(1))
    send_sums(0, 1)

    def z_copy(k, target, src, dst):
        return pltpu.make_async_remote_copy(
            src_ref=src, dst_ref=dst, send_sem=zsend_sem.at[0], recv_sem=zrecv_sem.at[k - 1],
            device_id=(peer(target),), device_id_type=MESH)

    for k in (6, 2, 4, 1):
        for v in range(2):
            z_copy(k, k, xbuf.at[v, pl.ds(0, batch)], zall.at[me, v]).start()

    def z_arrived(k):
        z_copy(k, k, zall.at[peer(k)], zall.at[peer(k)]).wait_recv()

    def relay(k):
        z_arrived(k)
        z_copy(k + 1, 1, zall.at[peer(k)], zall.at[peer(k)]).start()

    def prepare(k):
        d = peer(k)
        if k in (3, 5, 7, 1):
            z_arrived(k)
        sl = pl.ds(pl.multiple_of(d * batch, batch), batch)
        z = [xbuf[v, pl.ds(0, batch), :] if k == 0 else zall[d, v] for v in range(2)]
        for v in range(2):
            zt[:, pl.ds(pl.multiple_of((v * n + d) * batch, batch), batch)] = z[v].T
        x = jnp.concatenate(z, axis=0)
        p = None
        for jj in range(tiles // 2):
            s = lax.dot_general(x, cpad[pl.ds(jj * 256, 256), :], NT, preferred_element_type=F32)
            for h in range(2):
                j = 2 * jj + h
                sj = s[:, h * LANES:(h + 1) * LANES]
                e = jnp.exp2(sj * scale10)
                if j == tiles - 1:
                    e = e * tail_mask
                a = e * e
                for v in range(2):
                    half = slice(v * batch, (v + 1) * batch)
                    aall[v, j, sl, :] = a[half]
                    pall[v, j, sl, :] = e[half]
                    sall[v, j, sl, :] = sj[half]
                p = e if p is None else p + e
        r = jnp.sum(p, axis=1, keepdims=True)
        inv = coef / r
        lse_sum[d] = fold(jnp.broadcast_to(jnp.log(r), (2 * batch, LANES)))
        for v in range(2):
            for j in range(tiles):
                pall[v, j, sl, :] = pall[v, j, sl, :] * inv[v * batch:(v + 1) * batch]

    prepare(0)
    for v in range(2):
        col_scale(0, v)
        publish(1, v, sink_pass(v))
        send_sums(1, v)

    prepare(1)
    for k in (2, 4, 6):
        relay(k)
    for k in (2, 4):
        prepare(k)
    for v in range(2):
        col_scale(1, v)
        publish(2, v, sink_pass(v))
        send_sums(2, v)
    for k in (6, 3, 5, 7):
        prepare(k)


    def row_scale(v):
        w = [small[v, j:j + 1, :] for j in range(tiles)]

        def sums(d):
            sl = pl.ds(d * batch, batch)
            p = None
            m = None
            for j in range(tiles):
                t = aall[v, j, sl, :] * w[j]
                u = t * sall[1 - v, j, sl, :]
                p = t if p is None else p + t
                m = u if m is None else m + u
            return jnp.sum(p, axis=1, keepdims=True), m

        def scale(d, p, m):
            inv = 1.0 / p
            rinv[v, pl.ds(d * batch, batch), :] = jnp.broadcast_to(inv, (batch, LANES))
            return fold(m * inv)

        part = jnp.zeros((8, LANES), F32)
        last = None
        for d in range(n):
            this = sums(d)
            if d > 0:
                part = part + scale(d - 1, *last)
            last = this
        return part + scale(n - 1, *last)

    col_scale(2, 0)
    part = row_scale(0)
    col_scale(2, 1)
    small[2] = part + row_scale(1)

    for v in range(2):
        all_sums(2, v).wait_send()
    z_copy(1, 1, zall.at[pl.ds(0, n - 1)], zall.at[pl.ds(0, n - 1)]).wait_send()


def grads_kernel(
    n, protos, batch,
    aall, pall, rinv, zt, cpad, small, lse_sum,
    codes1_hbm, codes2_hbm, loss_ref, dz1_hbm, dz2_hbm, gp_hbm,
    gbuf, codes, gp, dz, out_sem,
):
    tiles = cpad.shape[0] // LANES
    batch_total = n * batch
    coef = 1.0 / (2 * batch_total * TEMPERATURE)
    me = lax.axis_index("data")
    own = pl.ds(pl.multiple_of(me * batch, batch), batch)
    codes_hbm = (codes1_hbm, codes2_hbm)
    dz_hbm = (dz1_hbm, dz2_hbm)

    pairs = tiles // 2
    deep = 2 * batch

    def cols_of(jj):
        return pl.ds(jj * 2 * LANES, min(2 * LANES, protos - jj * 2 * LANES))

    def body(acc, dz_acc):
        for ref in (*acc[0], *acc[1], dz_acc):
            pltpu.matmul_pop(ref)

        def tile(jj, v):
            w = [small[v, 2 * jj + h:2 * jj + h + 1, :] * coef for h in range(2)]
            for d in range(0, n, 2):
                halves = []
                for h in range(2):
                    sl = pl.ds(d * batch, deep)
                    j = 2 * jj + h
                    g = pall[1 - v, j, sl, :] - aall[v, j, sl, :] * w[h] * rinv[v, sl, :]
                    halves.append(g.astype(BF16))
                g = jnp.concatenate(halves, axis=1)
                gbuf[jj % 2, pl.ds((1 - v) * n * batch + d * batch, deep), :] = g
                unit = (d // 2) % 2
                pltpu.matmul_push_rhs(g, staging_register=0, mxu_index=unit)
                pltpu.matmul_acc_lhs(
                    acc[jj % 2][unit], zt[:, pl.ds((1 - v) * n * batch + d * batch, deep)], load_staged_rhs=0)

        def own_part(jj):
            for v in range(2):
                for h in range(2):
                    j = 2 * jj + h
                    part = min(LANES, protos - j * LANES)
                    q = aall[v, j, own, :] * small[v, j:j + 1, :] * rinv[v, own, :]
                    codes[v, pl.ds(j * LANES, part), :] = q.T[:part]
            c = cpad[pl.ds(jj * 2 * LANES, 2 * LANES), :]
            pltpu.matmul_push_rhs(jnp.concatenate([c, c], axis=1), staging_register=1, mxu_index=0)
            g = jnp.concatenate(
                [gbuf[jj % 2, pl.ds(pl.multiple_of((v * n + me) * batch, batch), batch), :] for v in range(2)], axis=0)
            pltpu.matmul_acc_lhs(dz_acc, g, load_staged_rhs=1)

        def drain(jj):
            g = pltpu.matmul_pop(acc[jj % 2][0]) + pltpu.matmul_pop(acc[jj % 2][1])
            cols = cols_of(jj)
            gp[cols, :] = g.T[:cols.size]

        def send(jj):
            cols = cols_of(jj)
            pltpu.make_async_copy(gp.at[cols], gp_hbm.at[cols], out_sem.at[4]).start()
            for v in range(2):
                pltpu.make_async_copy(codes.at[v, cols], codes_hbm[v].at[cols], out_sem.at[v]).start()

        for jj in range(pairs):
            tile(jj, 0)
            if jj > 0:
                drain(jj - 1)
            tile(jj, 1)
            own_part(jj)
            if jj > 0:
                send(jj - 1)
        drain(pairs - 1)
        send(pairs - 1)
        o = pltpu.matmul_pop(dz_acc)
        for v in range(2):
            dz[v] = o[v * batch:(v + 1) * batch, :LANES]
            pltpu.make_async_copy(dz.at[v], dz_hbm[v], out_sem.at[2 + v]).start()

    half = lambda unit: pltpu.ACC(unit)((LANES, 2 * LANES), F32)
    pl.run_scoped(body, ((half(0), half(1)), (half(0), half(1))), pltpu.ACC(0)((deep, 2 * LANES), F32))

    logs = lse_sum[0]
    for d in range(1, n):
        logs = logs + lse_sum[d]
    total = jnp.sum(small[2]) * (1.0 / TEMPERATURE) - jnp.sum(logs) * (1.0 / LANES)
    loss_ref[0, 0] = total * (-1.0 / (2 * batch_total))

    for v in range(2):
        pltpu.make_async_copy(codes.at[v, pl.ds(0, protos)], codes_hbm[v], out_sem.at[v]).wait()
        pltpu.make_async_copy(dz.at[v], dz_hbm[v], out_sem.at[2 + v]).wait()
    pltpu.make_async_copy(gp.at[pl.ds(0, protos)], gp_hbm, out_sem.at[4]).wait()


def solution(mesh):
    n = mesh.shape["data"]

    def local_step(z_one, z_two, protos, queue_one, queue_two):
        k, width = protos.shape
        batch, queue = z_one.shape[0], queue_one.shape[0]
        rows = batch + queue
        pad = (k + 255) // 256 * 256
        tiles = pad // LANES
        anywhere = pl.BlockSpec(memory_space=pl.ANY)
        sem = pltpu.SemaphoreType.DMA
        vmem = pl.BlockSpec(memory_space=pltpu.VMEM)
        whole = n * batch
        shared = pl.pallas_call(
            functools.partial(sums_kernel, n, k, batch, queue),
            out_shape=(
                pltpu.VMEM((2, tiles, whole, LANES), F32),
                pltpu.VMEM((2, tiles, whole, LANES), F32),
                pltpu.VMEM((2, whole, LANES), F32),
                pltpu.VMEM((width, 2 * whole), BF16),
                pltpu.VMEM((pad, width), BF16),
                pltpu.VMEM((4, tiles, LANES), F32),
                pltpu.VMEM((n, 8, LANES), F32),
            ),
            in_specs=[anywhere] * 5,
            out_specs=(vmem,) * 7,
            scratch_shapes=[
                pltpu.VMEM((2, rows, width), BF16),
                pltpu.VMEM((n, 2, batch, width), BF16),
                pltpu.VMEM((2, tiles, whole, LANES), F32),
                pltpu.VMEM((2, tiles, rows, LANES), F32),
                pltpu.VMEM((2, 8 * tiles, LANES), F32),
                pltpu.VMEM((ROUNDS, 2, n, tiles, LANES), F32),
                sem((3,)),
                sem((2,)),
                sem((ROUNDS, 2)),
                sem((1,)),
                sem((n - 1,)),
            ],
            compiler_params=pltpu.CompilerParams(
                collective_id=0, has_side_effects=True, vmem_limit_bytes=20 << 20),
            name="sums",
        )(*(pltpu.with_memory_space_constraint(x, pltpu.HBM) for x in (z_one, z_two, protos, queue_one, queue_two)))
        codes_one, codes_two, loss, dz_one, dz_two, grad_protos = pl.pallas_call(
            functools.partial(grads_kernel, n, k, batch),
            out_shape=(
                jax.ShapeDtypeStruct((k, batch), F32),
                jax.ShapeDtypeStruct((k, batch), F32),
                jax.ShapeDtypeStruct((1, 1), F32),
                jax.ShapeDtypeStruct((batch, width), F32),
                jax.ShapeDtypeStruct((batch, width), F32),
                jax.ShapeDtypeStruct((k, width), F32),
            ),
            in_specs=[vmem] * 7,
            out_specs=(anywhere, anywhere, pl.BlockSpec(memory_space=pltpu.SMEM), anywhere, anywhere, anywhere),
            scratch_shapes=[
                pltpu.VMEM((2, 2 * whole, 2 * LANES), BF16),
                pltpu.VMEM((2, pad, batch), F32),
                pltpu.VMEM((pad, width), F32),
                pltpu.VMEM((2, batch, width), F32),
                sem((5,)),
            ],
            compiler_params=pltpu.CompilerParams(vmem_limit_bytes=14 << 20),
            name="grads",
        )(*shared)
        return codes_one.T, codes_two.T, loss[0, 0], dz_one, dz_two, grad_protos

    row_spec = P("data", None)
    full_spec = P(None, None)
    return jax.shard_map(
        local_step,
        mesh=mesh,
        in_specs=(row_spec, row_spec, full_spec, row_spec, row_spec),
        out_specs=(row_spec, row_spec, P(), row_spec, row_spec, full_spec),
        check_vma=False,
    )
```

```python
import functools
import math

import jax
import jax.numpy as jnp
from jax import lax
from jax.experimental import pallas as pl
from jax.experimental.pallas import tpu as pltpu
from jax.sharding import PartitionSpec as P

EPSILON = 0.05
TEMPERATURE = 0.1
ROUNDS = 3
LANES = 128
MESH = pl.DeviceIdType.MESH
F32 = jnp.float32
BF16 = jnp.bfloat16
NT = (((1,), (1,)), ((), ()))


def fold(x):
    return jnp.sum(x.reshape(x.shape[0] // 8, 8, LANES), axis=0)


def sums_kernel(
    n, protos, batch, queue,
    z1_hbm, z2_hbm, c_hbm, q1_hbm, q2_hbm,
    aall, pall, rinv, zt, cpad, small, lse_sum,
    xbuf, zall, sall, atr, cpart, csum,
    in_sem, send_sem, recv_sem, zsend_sem, zrecv_sem,
):
    tiles = cpad.shape[0] // LANES
    rows = batch + queue
    total_rows = n * rows
    coef = 1.0 / (2 * n * batch * TEMPERATURE)
    scale10 = math.log2(math.e) / TEMPERATURE

    me = lax.axis_index("data")
    bit0 = lax.rem(me, 2)
    bit1 = lax.rem(me // 2, 2)
    bit2 = me // 4

    def peer(k):
        b0, b1, b2 = k % 2, (k // 2) % 2, k // 4
        return (lax.rem(bit2 + b2, 2) * 2 + lax.rem(bit1 + b1, 2)) * 2 + lax.rem(bit0 + b0, 2)

    far_first = (6, 7, 4, 5, 2, 3, 1)

    c_in = pltpu.make_async_copy(c_hbm, cpad.at[pl.ds(0, protos)], in_sem.at[2])

    def rows_in(v):
        z_hbm, q_hbm = ((z1_hbm, q1_hbm), (z2_hbm, q2_hbm))[v]
        pltpu.make_async_copy(z_hbm, xbuf.at[v, pl.ds(0, batch)], in_sem.at[v]).start()
        pltpu.make_async_copy(q_hbm, xbuf.at[v, pl.ds(batch, queue)], in_sem.at[v]).start()

    def wait_rows(v):
        pltpu.make_async_copy(xbuf.at[v], xbuf.at[v], in_sem.at[v]).wait()

    c_in.start()
    rows_in(0)
    rows_in(1)

    barrier = pltpu.get_barrier_semaphore()
    for k in far_first:
        pl.semaphore_signal(barrier, inc=1, device_id=(peer(k),), device_id_type=MESH)

    cpad[pl.ds(protos, cpad.shape[0] - protos), :] = jnp.zeros((cpad.shape[0] - protos, LANES), BF16)
    c_in.wait()

    lane = lax.broadcasted_iota(jnp.int32, (1, LANES), 1)
    tail_ok = lane < (protos - (tiles - 1) * LANES)
    tail_mask = tail_ok.astype(F32)

    def publish(t, v, acc):
        for j in range(tiles):
            cpart[v, pl.ds(8 * j, 8), :] = acc[j]
        out = cpart[v, pl.ds(0, tiles, stride=8), :]
        for s in range(1, 8):
            out = out + cpart[v, pl.ds(s, tiles, stride=8), :]
        csum[t, v, me] = out

    def sum_copy(t, v, k, slots):
        return pltpu.make_async_remote_copy(
            src_ref=csum.at[t, v, slots], dst_ref=csum.at[t, v, slots],
            send_sem=send_sem.at[v], recv_sem=recv_sem.at[t, v],
            device_id=(peer(k),), device_id_type=MESH)

    def all_sums(t, v):
        return sum_copy(t, v, 1, pl.ds(0, n - 1))

    def send_sums(t, v):
        if t > 0:
            all_sums(t, v).wait_send()
        for k in far_first:
            sum_copy(t, v, k, me).start()

    def col_scale(t, v):
        all_sums(t, v).wait_recv()
        c = csum[t, v, 0]
        for d in range(1, n):
            c = c + csum[t, v, d]
        w = 1.0 / (protos * c)
        index = (lax.broadcasted_iota(jnp.int32, (tiles, LANES), 0) * LANES
                 + lax.broadcasted_iota(jnp.int32, (tiles, LANES), 1))
        small[v] = jnp.where(index < protos, w, 0.0)

    def first_pass(v):
        acc = [jnp.zeros((8, LANES), F32) for _ in range(tiles)]
        for start, size in ((0, rows // 2), (rows // 2, rows // 2)):
            x = xbuf[v, pl.ds(start, size), :]
            for jj in range(tiles // 2):
                s = lax.dot_general(x, cpad[pl.ds(jj * 256, 256), :], NT, preferred_element_type=F32)
                for h in range(2):
                    e = jnp.exp2(s[:, h * LANES:(h + 1) * LANES] * scale10)
                    a = e * e
                    atr[v, 2 * jj + h, pl.ds(start, size), :] = a
                    acc[2 * jj + h] = acc[2 * jj + h] + fold(a)
        return acc

    def sink_pass(v):
        acc = [jnp.zeros((8, LANES), F32) for _ in range(tiles)]
        step = 128
        for b in range(rows // step):
            sl = pl.ds(b * step, step)
            p = atr[v, 0, sl, :] * small[v, 0:1, :]
            for j in range(1, tiles):
                p = p + atr[v, j, sl, :] * small[v, j:j + 1, :]
            u = 1.0 / (total_rows * jnp.sum(p, axis=1, keepdims=True))
            for j in range(tiles):
                acc[j] = acc[j] + fold(atr[v, j, sl, :] * u)
        return acc

    wait_rows(0)
    publish(0, 0, first_pass(0))
    pl.semaphore_wait(barrier, n - 1)
    send_sums(0, 0)
    wait_rows(1)
    publish(0, 1, first_pass(1))
    send_sums(0, 1)

    def z_copy(k, target, src, dst):
        return pltpu.make_async_remote_copy(
            src_ref=src, dst_ref=dst, send_sem=zsend_sem.at[0], recv_sem=zrecv_sem.at[k - 1],
            device_id=(peer(target),), device_id_type=MESH)

    for k in (6, 2, 4, 1):
        for v in range(2):
            z_copy(k, k, xbuf.at[v, pl.ds(0, batch)], zall.at[me, v]).start()

    def z_arrived(k):
        z_copy(k, k, zall.at[peer(k)], zall.at[peer(k)]).wait_recv()

    def relay(k):
        z_arrived(k)
        z_copy(k + 1, 1, zall.at[peer(k)], zall.at[peer(k)]).start()

    def prepare(k):
        d = peer(k)
        if k in (3, 5, 7, 1):
            z_arrived(k)
        sl = pl.ds(pl.multiple_of(d * batch, batch), batch)
        z = [xbuf[v, pl.ds(0, batch), :] if k == 0 else zall[d, v] for v in range(2)]
        for v in range(2):
            zt[:, pl.ds(pl.multiple_of((v * n + d) * batch, batch), batch)] = z[v].astype(F32).T
        x = jnp.concatenate(z, axis=0)
        p = None
        for jj in range(tiles // 2):
            s = lax.dot_general(x, cpad[pl.ds(jj * 256, 256), :], NT, preferred_element_type=F32)
            for h in range(2):
                j = 2 * jj + h
                sj = s[:, h * LANES:(h + 1) * LANES]
                e = jnp.exp2(sj * scale10)
                if j == tiles - 1:
                    e = e * tail_mask
                a = e * e
                for v in range(2):
                    half = slice(v * batch, (v + 1) * batch)
                    aall[v, j, sl, :] = a[half]
                    pall[v, j, sl, :] = e[half]
                    sall[v, j, sl, :] = sj[half]
                p = e if p is None else p + e
        r = jnp.sum(p, axis=1, keepdims=True)
        inv = coef / r
        lse_sum[d] = fold(jnp.broadcast_to(jnp.log(r), (2 * batch, LANES)))
        for v in range(2):
            for j in range(tiles):
                pall[v, j, sl, :] = pall[v, j, sl, :] * inv[v * batch:(v + 1) * batch]

    prepare(0)
    for v in range(2):
        col_scale(0, v)
        publish(1, v, sink_pass(v))
        send_sums(1, v)

    prepare(1)
    for k in (2, 4, 6):
        relay(k)
    for k in (2, 4):
        prepare(k)
    for v in range(2):
        col_scale(1, v)
        publish(2, v, sink_pass(v))
        send_sums(2, v)
    for k in (6, 3, 5, 7):
        prepare(k)


    def row_scale(v):
        w = [small[v, j:j + 1, :] for j in range(tiles)]

        def sums(d):
            sl = pl.ds(d * batch, batch)
            p = None
            m = None
            for j in range(tiles):
                t = aall[v, j, sl, :] * w[j]
                aall[v, j, sl, :] = t
                u = t * sall[1 - v, j, sl, :]
                p = t if p is None else p + t
                m = u if m is None else m + u
            return jnp.sum(p, axis=1, keepdims=True), m

        def scale(d, p, m):
            inv = 1.0 / p
            rinv[v, pl.ds(d * batch, batch), :] = jnp.broadcast_to(coef * inv, (batch, LANES))
            return fold(m * inv)

        part = jnp.zeros((8, LANES), F32)
        last = None
        for d in range(n):
            this = sums(d)
            if d > 0:
                part = part + scale(d - 1, *last)
            last = this
        return part + scale(n - 1, *last)

    col_scale(2, 0)
    part = row_scale(0)
    col_scale(2, 1)
    small[2] = part + row_scale(1)

    for v in range(2):
        all_sums(2, v).wait_send()
    z_copy(1, 1, zall.at[pl.ds(0, n - 1)], zall.at[pl.ds(0, n - 1)]).wait_send()


def grads_kernel(
    n, protos, batch,
    aall, pall, rinv, zt, cpad, small, lse_sum,
    codes1_hbm, codes2_hbm, loss_hbm, dz1_hbm, dz2_hbm, gp_hbm,
    codes, gp, dz, loss, out_sem,
):
    tiles = cpad.shape[0] // LANES
    batch_total = n * batch
    coef = 1.0 / (2 * batch_total * TEMPERATURE)
    me = lax.axis_index("data")
    own = pl.ds(pl.multiple_of(me * batch, batch), batch)
    codes_hbm = (codes1_hbm, codes2_hbm)
    dz_hbm = (dz1_hbm, dz2_hbm)

    logs = lse_sum[0]
    for d in range(1, n):
        logs = logs + lse_sum[d]
    total = jnp.sum(small[2]) * (1.0 / TEMPERATURE) - jnp.sum(logs) * (1.0 / LANES)
    loss[0, 0] = total * (-1.0 / (2 * batch_total))
    pltpu.make_async_copy(loss, loss_hbm, out_sem.at[5]).start()

    pairs = tiles // 2
    deep = 2 * batch

    def cols_of(jj):
        return pl.ds(jj * 2 * LANES, min(2 * LANES, protos - jj * 2 * LANES))

    def body(acc, dz_acc):
        for ref in (*acc[0], *acc[1], *dz_acc):
            pltpu.matmul_pop(ref)

        def tiles_of(big, v):
            for d in range(0, n, 2):
                sl = pl.ds(d * batch, deep)
                scale = rinv[v, sl, :]
                lhs = zt[:, pl.ds((1 - v) * n * batch + d * batch, deep)]
                reg = (d // 2) % 2
                for unit in range(2):
                    g = [pall[1 - v, j, sl, :] - aall[v, j, sl, :] * scale
                         for j in (4 * big + 2 * unit, 4 * big + 2 * unit + 1)]
                    pltpu.matmul_push_rhs(jnp.concatenate(g, axis=1), staging_register=reg, mxu_index=unit)
                    pltpu.matmul_acc_lhs(acc[big][unit], lhs, load_staged_rhs=reg)

        def own_part(jj):
            lhs = []
            for v in range(2):
                g = []
                for h in range(2):
                    j = 2 * jj + h
                    part = min(LANES, protos - j * LANES)
                    q = aall[v, j, own, :] * rinv[v, own, :]
                    g.append(pall[1 - v, j, own, :] - q)
                    codes[v, pl.ds(j * LANES, part), :] = (q * (1.0 / coef)).T[:part]
                lhs.insert(0, jnp.concatenate(g, axis=1))
            c = cpad[pl.ds(jj * 2 * LANES, 2 * LANES), :].astype(F32)
            pltpu.matmul_push_rhs(jnp.concatenate([c, c], axis=1), staging_register=0, mxu_index=jj % 2)
            pltpu.matmul_acc_lhs(dz_acc[jj % 2], jnp.concatenate(lhs, axis=0), load_staged_rhs=0)

        def drain(big):
            for unit in range(2):
                cols = cols_of(2 * big + unit)
                gp[cols, :] = pltpu.matmul_pop(acc[big][unit]).T[:cols.size]

        def send(big):
            for jj in (2 * big, 2 * big + 1):
                cols = cols_of(jj)
                pltpu.make_async_copy(gp.at[cols], gp_hbm.at[cols], out_sem.at[4]).start()

        def send_codes(big):
            for jj in (2 * big, 2 * big + 1):
                cols = cols_of(jj)
                for v in range(2):
                    pltpu.make_async_copy(codes.at[v, cols], codes_hbm[v].at[cols], out_sem.at[v]).start()

        own_part(0)
        own_part(1)
        send_codes(0)
        tiles_of(0, 0)
        tiles_of(0, 1)
        own_part(2)
        own_part(3)
        send_codes(1)
        tiles_of(1, 0)
        drain(0)
        send(0)
        o = pltpu.matmul_pop(dz_acc[0]) + pltpu.matmul_pop(dz_acc[1])
        for v in range(2):
            dz[v] = o[v * batch:(v + 1) * batch, :LANES]
            pltpu.make_async_copy(dz.at[v], dz_hbm[v], out_sem.at[2 + v]).start()
        tiles_of(1, 1)
        drain(1)
        send(1)

    def acc_of(rows):
        return tuple(pltpu.ACC(unit)((rows, 2 * LANES), F32) for unit in range(2))

    pl.run_scoped(body, (acc_of(LANES), acc_of(LANES)), acc_of(deep))

    for v in range(2):
        pltpu.make_async_copy(codes.at[v, pl.ds(0, protos)], codes_hbm[v], out_sem.at[v]).wait()
        pltpu.make_async_copy(dz.at[v], dz_hbm[v], out_sem.at[2 + v]).wait()
    pltpu.make_async_copy(gp.at[pl.ds(0, protos)], gp_hbm, out_sem.at[4]).wait()
    pltpu.make_async_copy(loss, loss_hbm, out_sem.at[5]).wait()


def solution(mesh):
    n = mesh.shape["data"]

    def local_step(z_one, z_two, protos, queue_one, queue_two):
        k, width = protos.shape
        batch, queue = z_one.shape[0], queue_one.shape[0]
        rows = batch + queue
        pad = (k + 255) // 256 * 256
        tiles = pad // LANES
        anywhere = pl.BlockSpec(memory_space=pl.ANY)
        sem = pltpu.SemaphoreType.DMA
        vmem = pl.BlockSpec(memory_space=pltpu.VMEM)
        whole = n * batch
        shared = pl.pallas_call(
            functools.partial(sums_kernel, n, k, batch, queue),
            out_shape=(
                pltpu.VMEM((2, tiles, whole, LANES), F32),
                pltpu.VMEM((2, tiles, whole, LANES), F32),
                pltpu.VMEM((2, whole, LANES), F32),
                pltpu.VMEM((width, 2 * whole), F32),
                pltpu.VMEM((pad, width), BF16),
                pltpu.VMEM((4, tiles, LANES), F32),
                pltpu.VMEM((n, 8, LANES), F32),
            ),
            in_specs=[anywhere] * 5,
            out_specs=(vmem,) * 7,
            scratch_shapes=[
                pltpu.VMEM((2, rows, width), BF16),
                pltpu.VMEM((n, 2, batch, width), BF16),
                pltpu.VMEM((2, tiles, whole, LANES), F32),
                pltpu.VMEM((2, tiles, rows, LANES), F32),
                pltpu.VMEM((2, 8 * tiles, LANES), F32),
                pltpu.VMEM((ROUNDS, 2, n, tiles, LANES), F32),
                sem((3,)),
                sem((2,)),
                sem((ROUNDS, 2)),
                sem((1,)),
                sem((n - 1,)),
            ],
            compiler_params=pltpu.CompilerParams(
                collective_id=0, has_side_effects=True, vmem_limit_bytes=20 << 20),
            name="sums",
        )(*(pltpu.with_memory_space_constraint(x, pltpu.HBM) for x in (z_one, z_two, protos, queue_one, queue_two)))
        codes_one, codes_two, loss, dz_one, dz_two, grad_protos = pl.pallas_call(
            functools.partial(grads_kernel, n, k, batch),
            out_shape=(
                jax.ShapeDtypeStruct((k, batch), F32),
                jax.ShapeDtypeStruct((k, batch), F32),
                jax.ShapeDtypeStruct((1, 1), F32),
                jax.ShapeDtypeStruct((batch, width), F32),
                jax.ShapeDtypeStruct((batch, width), F32),
                jax.ShapeDtypeStruct((k, width), F32),
            ),
            in_specs=[vmem] * 7,
            out_specs=(anywhere,) * 6,
            scratch_shapes=[
                pltpu.VMEM((2, pad, batch), F32),
                pltpu.VMEM((pad, width), F32),
                pltpu.VMEM((2, batch, width), F32),
                pltpu.SMEM((1, 1), F32),
                sem((6,)),
            ],
            compiler_params=pltpu.CompilerParams(vmem_limit_bytes=14 << 20),
            name="grads",
        )(*shared)
        return codes_one.T, codes_two.T, loss[0, 0], dz_one, dz_two, grad_protos

    row_spec = P("data", None)
    full_spec = P(None, None)
    return jax.shard_map(
        local_step,
        mesh=mesh,
        in_specs=(row_spec, row_spec, full_spec, row_spec, row_spec),
        out_specs=(row_spec, row_spec, P(), row_spec, row_spec, full_spec),
        check_vma=False,
    )
```

```python
import functools
import math

import jax
import jax.numpy as jnp
from jax import lax
from jax.experimental import pallas as pl
from jax.experimental.pallas import tpu as pltpu
from jax.sharding import PartitionSpec as P

EPSILON = 0.05
TEMPERATURE = 0.1
ROUNDS = 3
LANES = 128
MESH = pl.DeviceIdType.MESH
F32 = jnp.float32
BF16 = jnp.bfloat16
NT = (((1,), (1,)), ((), ()))


def fold(x):
    return jnp.sum(x.reshape(x.shape[0] // 8, 8, LANES), axis=0)


def sums_kernel(
    n, protos, batch, queue,
    z1_hbm, z2_hbm, c_hbm, q1_hbm, q2_hbm,
    aall, pall, rinv, zt, cpad, small, lse_sum,
    xbuf, zall, sall, atr, cpart, csum,
    sem, recv_sem, zrecv_sem,
):
    tiles = cpad.shape[0] // LANES
    rows = batch + queue
    total_rows = n * rows
    coef = 1.0 / (2 * n * batch * TEMPERATURE)
    scale10 = math.log2(math.e) / TEMPERATURE
    scale20 = math.log2(math.e) / EPSILON

    me = lax.axis_index("data")
    bit0 = lax.rem(me, 2)
    bit1 = lax.rem(me // 2, 2)
    bit2 = me // 4

    def peer(k):
        b0, b1, b2 = k % 2, (k // 2) % 2, k // 4
        return (lax.rem(bit2 + b2, 2) * 2 + lax.rem(bit1 + b1, 2)) * 2 + lax.rem(bit0 + b0, 2)

    far_first = (6, 7, 4, 5, 2, 3, 1)

    barrier = pltpu.get_barrier_semaphore()
    for k in far_first:
        pl.semaphore_signal(barrier, inc=1, device_id=(peer(k),), device_id_type=MESH)

    c_in = pltpu.make_async_copy(c_hbm, cpad.at[pl.ds(0, protos)], sem.at[2])

    def rows_in(v):
        z_hbm, q_hbm = ((z1_hbm, q1_hbm), (z2_hbm, q2_hbm))[v]
        pltpu.make_async_copy(z_hbm, xbuf.at[v, pl.ds(0, batch)], sem.at[v]).start()
        pltpu.make_async_copy(q_hbm, xbuf.at[v, pl.ds(batch, queue)], sem.at[v]).start()

    def wait_rows(v):
        pltpu.make_async_copy(xbuf.at[v], xbuf.at[v], sem.at[v]).wait()

    c_in.start()
    rows_in(0)
    rows_in(1)

    cpad[pl.ds(protos, cpad.shape[0] - protos), :] = jnp.zeros((cpad.shape[0] - protos, LANES), BF16)
    c_in.wait()

    lane = lax.broadcasted_iota(jnp.int32, (1, LANES), 1)
    tail_ok = lane < (protos - (tiles - 1) * LANES)
    tail_mask = tail_ok.astype(F32)

    def publish(t, v, acc):
        for j in range(tiles):
            cpart[v, pl.ds(8 * j, 8), :] = acc[j]
        out = cpart[v, pl.ds(0, tiles, stride=8), :]
        for s in range(1, 8):
            out = out + cpart[v, pl.ds(s, tiles, stride=8), :]
        csum[t, v, me] = out

    def sum_copy(t, v, k, slots):
        return pltpu.make_async_remote_copy(
            src_ref=csum.at[t, v, slots], dst_ref=csum.at[t, v, slots],
            send_sem=sem.at[v], recv_sem=recv_sem.at[t % 2, v],
            device_id=(peer(k),), device_id_type=MESH)

    def all_sums(t, v):
        return sum_copy(t, v, 1, pl.ds(0, n - 1))

    def send_sums(t, v):
        if t > 0:
            all_sums(t, v).wait_send()
        for k in far_first:
            sum_copy(t, v, k, me).start()

    def col_scale(t, v):
        all_sums(t, v).wait_recv()
        c = csum[t, v, 0]
        for d in range(1, n):
            c = c + csum[t, v, d]
        w = 1.0 / (protos * c)
        index = (lax.broadcasted_iota(jnp.int32, (tiles, LANES), 0) * LANES
                 + lax.broadcasted_iota(jnp.int32, (tiles, LANES), 1))
        small[v] = jnp.where(index < protos, w, 0.0)

    def first_pass(v):
        acc = [jnp.zeros((8, LANES), F32) for _ in range(tiles)]
        for start, size in ((0, rows // 2), (rows // 2, rows // 2)):
            x = xbuf[v, pl.ds(start, size), :]
            for jj in range(tiles // 2):
                s = lax.dot_general(x, cpad[pl.ds(jj * 256, 256), :], NT, preferred_element_type=F32)
                for h in range(2):
                    a = jnp.exp2(s[:, h * LANES:(h + 1) * LANES] * scale20)
                    atr[v, 2 * jj + h, pl.ds(start, size), :] = a
                    acc[2 * jj + h] = acc[2 * jj + h] + fold(a)
        return acc

    def sink_pass(v):
        acc = [jnp.zeros((8, LANES), F32) for _ in range(tiles)]
        step = 128
        for b in range(rows // step):
            sl = pl.ds(b * step, step)
            p = atr[v, 0, sl, :] * small[v, 0:1, :]
            for j in range(1, tiles):
                p = p + atr[v, j, sl, :] * small[v, j:j + 1, :]
            u = 1.0 / (total_rows * jnp.sum(p, axis=1, keepdims=True))
            for j in range(tiles):
                acc[j] = acc[j] + fold(atr[v, j, sl, :] * u)
        return acc

    wait_rows(0)
    publish(0, 0, first_pass(0))
    pl.semaphore_wait(barrier, n - 1)
    send_sums(0, 0)
    wait_rows(1)
    publish(0, 1, first_pass(1))
    send_sums(0, 1)

    def z_copy(k, target, src, dst):
        return pltpu.make_async_remote_copy(
            src_ref=src, dst_ref=dst, send_sem=sem.at[2], recv_sem=zrecv_sem.at[(0, 1, 2, 3)[k // 2] if k in (1, 2, 4, 6) else 4],
            device_id=(peer(target),), device_id_type=MESH)

    for k in (1, 2, 4, 6):
        for v in range(2):
            z_copy(k, k, xbuf.at[v, pl.ds(0, batch)], zall.at[me, v]).start()

    def z_arrived(k):
        z_copy(k, k, zall.at[peer(k)], zall.at[peer(k)]).wait_recv()

    def relays_arrived(k):
        z_copy(3, 1, zall.at[pl.ds(0, 3)], zall.at[pl.ds(0, 3)]).wait_recv()

    def relay(k):
        z_arrived(k)
        z_copy(k + 1, 1, zall.at[peer(k)], zall.at[peer(k)]).start()

    def block_of(k):
        return pl.ds(pl.multiple_of(peer(k) * batch, batch), batch)

    def transport(k):
        d = peer(k)
        z = [xbuf[v, pl.ds(0, batch), :] if k == 0 else zall[d, v] for v in range(2)]
        for v in range(2):
            zt[:, pl.ds(pl.multiple_of((v * n + d) * batch, batch), batch)] = z[v].astype(F32).T
        x = jnp.concatenate(z, axis=0)
        p = None
        for jj in range(tiles // 2):
            s = lax.dot_general(x, cpad[pl.ds(jj * 256, 256), :], NT, preferred_element_type=F32)
            for h in range(2):
                j = 2 * jj + h
                sj = s[:, h * LANES:(h + 1) * LANES]
                e = jnp.exp2(sj * scale10)
                if j == tiles - 1:
                    e = e * tail_mask
                a = e * e
                for v in range(2):
                    half = slice(v * batch, (v + 1) * batch)
                    aall[v, j, block_of(k), :] = a[half]
                    pall[v, j, block_of(k), :] = e[half]
                    sall[v, j, block_of(k), :] = sj[half]
                p = e if p is None else p + e
        return jnp.sum(p, axis=1, keepdims=True)

    def softmax(k, r):
        lse_sum[peer(k)] = fold(jnp.broadcast_to(jnp.log(r), (2 * batch, LANES)))
        inv = coef / r
        for v in range(2):
            for j in range(tiles):
                pall[v, j, block_of(k), :] = pall[v, j, block_of(k), :] * inv[v * batch:(v + 1) * batch]

    def prepare(steps):
        last = None
        for k, before in steps:
            before(k)
            r = transport(k)
            if last is not None:
                softmax(*last)
            last = k, r
        softmax(*last)

    def ready(k):
        pass

    prepare([(0, ready), (1, z_arrived)])
    for v in range(2):
        col_scale(0, v)
        publish(1, v, sink_pass(v))
        send_sums(1, v)

    prepare([(2, relay), (4, relay)])
    relay(6)
    for v in range(2):
        col_scale(1, v)
        publish(2, v, sink_pass(v))
        send_sums(2, v)
    prepare([(6, ready), (3, relays_arrived), (5, ready), (7, ready)])

    def row_scale(v):
        w = [small[v, j:j + 1, :] for j in range(tiles)]

        def sums(d):
            sl = pl.ds(d * batch, batch)
            p = None
            m = None
            for j in range(tiles):
                t = aall[v, j, sl, :] * w[j]
                aall[v, j, sl, :] = t
                u = t * sall[1 - v, j, sl, :]
                p = t if p is None else p + t
                m = u if m is None else m + u
            return jnp.sum(p, axis=1, keepdims=True), m

        def scale(d, p, m):
            inv = 1.0 / p
            rinv[v, pl.ds(d * batch, batch), :] = jnp.broadcast_to(coef * inv, (batch, LANES))
            return fold(m * inv)

        part = jnp.zeros((8, LANES), F32)
        last = None
        for d in range(n):
            this = sums(d)
            if d > 0:
                part = part + scale(d - 1, *last)
            last = this
        return part + scale(n - 1, *last)

    col_scale(2, 0)
    part = row_scale(0)
    col_scale(2, 1)
    small[2] = part + row_scale(1)

    for v in range(2):
        all_sums(2, v).wait_send()
    z_copy(1, 1, zall.at[pl.ds(0, n - 1)], zall.at[pl.ds(0, n - 1)]).wait_send()


def grads_kernel(
    n, protos, batch,
    aall, pall, rinv, zt, cpad, small, lse_sum,
    codes1_hbm, codes2_hbm, loss_hbm, dz1_hbm, dz2_hbm, gp_hbm,
    codes, gp, dz, loss, out_sem,
):
    tiles = cpad.shape[0] // LANES
    batch_total = n * batch
    coef = 1.0 / (2 * batch_total * TEMPERATURE)
    me = lax.axis_index("data")
    own = pl.ds(pl.multiple_of(me * batch, batch), batch)
    codes_hbm = (codes1_hbm, codes2_hbm)
    dz_hbm = (dz1_hbm, dz2_hbm)

    logs = lse_sum[0]
    for d in range(1, n):
        logs = logs + lse_sum[d]
    total = jnp.sum(small[2]) * (1.0 / TEMPERATURE) - jnp.sum(logs) * (1.0 / LANES)
    loss[0, 0] = total * (-1.0 / (2 * batch_total))
    pltpu.make_async_copy(loss, loss_hbm, out_sem.at[5]).start()

    pairs = tiles // 2
    deep = 2 * batch

    def cols_of(jj):
        return pl.ds(jj * 2 * LANES, min(2 * LANES, protos - jj * 2 * LANES))

    def body(acc, dz_acc):
        for ref in (*acc[0], *acc[1], *dz_acc):
            pltpu.matmul_pop(ref)

        def tiles_of(big, v):
            for d in range(0, n, 2):
                sl = pl.ds(d * batch, deep)
                scale = rinv[v, sl, :]
                lhs = zt[:, pl.ds((1 - v) * n * batch + d * batch, deep)]
                reg = (d // 2) % 2
                for unit in range(2):
                    g = [pall[1 - v, j, sl, :] - aall[v, j, sl, :] * scale
                         for j in (4 * big + 2 * unit, 4 * big + 2 * unit + 1)]
                    pltpu.matmul_push_rhs(jnp.concatenate(g, axis=1), staging_register=reg, mxu_index=unit)
                    pltpu.matmul_acc_lhs(acc[big][unit], lhs, load_staged_rhs=reg)

        def own_part(jj):
            lhs = []
            for v in range(2):
                g = []
                for h in range(2):
                    j = 2 * jj + h
                    part = min(LANES, protos - j * LANES)
                    q = aall[v, j, own, :] * rinv[v, own, :]
                    g.append(pall[1 - v, j, own, :] - q)
                    codes[v, pl.ds(j * LANES, part), :] = (q * (1.0 / coef)).T[:part]
                lhs.insert(0, jnp.concatenate(g, axis=1))
            c = cpad[pl.ds(jj * 2 * LANES, 2 * LANES), :].astype(F32)
            pltpu.matmul_push_rhs(jnp.concatenate([c, c], axis=1), staging_register=0, mxu_index=jj % 2)
            pltpu.matmul_acc_lhs(dz_acc[jj % 2], jnp.concatenate(lhs, axis=0), load_staged_rhs=0)

        def drain(big):
            for unit in range(2):
                cols = cols_of(2 * big + unit)
                gp[cols, :] = pltpu.matmul_pop(acc[big][unit]).T[:cols.size]

        def send(big):
            for jj in (2 * big, 2 * big + 1):
                cols = cols_of(jj)
                pltpu.make_async_copy(gp.at[cols], gp_hbm.at[cols], out_sem.at[4]).start()

        def send_codes(big):
            for jj in (2 * big, 2 * big + 1):
                cols = cols_of(jj)
                for v in range(2):
                    pltpu.make_async_copy(codes.at[v, cols], codes_hbm[v].at[cols], out_sem.at[v]).start()

        own_part(0)
        own_part(1)
        send_codes(0)
        tiles_of(0, 0)
        tiles_of(0, 1)
        own_part(2)
        own_part(3)
        send_codes(1)
        tiles_of(1, 0)
        drain(0)
        send(0)
        o = pltpu.matmul_pop(dz_acc[0]) + pltpu.matmul_pop(dz_acc[1])
        for v in range(2):
            dz[v] = o[v * batch:(v + 1) * batch, :LANES]
            pltpu.make_async_copy(dz.at[v], dz_hbm[v], out_sem.at[2 + v]).start()
        tiles_of(1, 1)
        drain(1)
        send(1)

    def acc_of(rows):
        return tuple(pltpu.ACC(unit)((rows, 2 * LANES), F32) for unit in range(2))

    pl.run_scoped(body, (acc_of(LANES), acc_of(LANES)), acc_of(deep))

    for v in range(2):
        pltpu.make_async_copy(codes.at[v, pl.ds(0, protos)], codes_hbm[v], out_sem.at[v]).wait()
        pltpu.make_async_copy(dz.at[v], dz_hbm[v], out_sem.at[2 + v]).wait()
    pltpu.make_async_copy(gp.at[pl.ds(0, protos)], gp_hbm, out_sem.at[4]).wait()
    pltpu.make_async_copy(loss, loss_hbm, out_sem.at[5]).wait()


def solution(mesh):
    n = mesh.shape["data"]

    def local_step(z_one, z_two, protos, queue_one, queue_two):
        k, width = protos.shape
        batch, queue = z_one.shape[0], queue_one.shape[0]
        rows = batch + queue
        pad = (k + 255) // 256 * 256
        tiles = pad // LANES
        anywhere = pl.BlockSpec(memory_space=pl.ANY)
        sem = pltpu.SemaphoreType.DMA
        vmem = pl.BlockSpec(memory_space=pltpu.VMEM)
        whole = n * batch
        shared = pl.pallas_call(
            functools.partial(sums_kernel, n, k, batch, queue),
            out_shape=(
                pltpu.VMEM((2, tiles, whole, LANES), F32),
                pltpu.VMEM((2, tiles, whole, LANES), F32),
                pltpu.VMEM((2, whole, LANES), F32),
                pltpu.VMEM((width, 2 * whole), F32),
                pltpu.VMEM((pad, width), BF16),
                pltpu.VMEM((4, tiles, LANES), F32),
                pltpu.VMEM((n, 8, LANES), F32),
            ),
            in_specs=[anywhere] * 5,
            out_specs=(vmem,) * 7,
            scratch_shapes=[
                pltpu.VMEM((2, rows, width), BF16),
                pltpu.VMEM((n, 2, batch, width), BF16),
                pltpu.VMEM((2, tiles, whole, LANES), F32),
                pltpu.VMEM((2, tiles, rows, LANES), F32),
                pltpu.VMEM((2, 8 * tiles, LANES), F32),
                pltpu.VMEM((ROUNDS, 2, n, tiles, LANES), F32),
                sem((3,)),
                sem((2, 2)),
                sem((5,)),
            ],
            compiler_params=pltpu.CompilerParams(
                collective_id=0, has_side_effects=True, vmem_limit_bytes=20 << 20),
            name="sums",
        )(*(pltpu.with_memory_space_constraint(x, pltpu.HBM) for x in (z_one, z_two, protos, queue_one, queue_two)))
        codes_one, codes_two, loss, dz_one, dz_two, grad_protos = pl.pallas_call(
            functools.partial(grads_kernel, n, k, batch),
            out_shape=(
                jax.ShapeDtypeStruct((k, batch), F32),
                jax.ShapeDtypeStruct((k, batch), F32),
                jax.ShapeDtypeStruct((1, 1), F32),
                jax.ShapeDtypeStruct((batch, width), F32),
                jax.ShapeDtypeStruct((batch, width), F32),
                jax.ShapeDtypeStruct((k, width), F32),
            ),
            in_specs=[vmem] * 7,
            out_specs=(anywhere,) * 6,
            scratch_shapes=[
                pltpu.VMEM((2, pad, batch), F32),
                pltpu.VMEM((pad, width), F32),
                pltpu.VMEM((2, batch, width), F32),
                pltpu.SMEM((1, 1), F32),
                sem((6,)),
            ],
            compiler_params=pltpu.CompilerParams(vmem_limit_bytes=14 << 20),
            name="grads",
        )(*shared)
        return codes_one.T, codes_two.T, loss[0, 0], dz_one, dz_two, grad_protos

    row_spec = P("data", None)
    full_spec = P(None, None)
    return jax.shard_map(
        local_step,
        mesh=mesh,
        in_specs=(row_spec, row_spec, full_spec, row_spec, row_spec),
        out_specs=(row_spec, row_spec, P(), row_spec, row_spec, full_spec),
        check_vma=False,
    )
```

```python
import functools
import math

import jax
import jax.numpy as jnp
from jax import lax
from jax.experimental import pallas as pl
from jax.experimental.pallas import tpu as pltpu
from jax.sharding import PartitionSpec as P

EPSILON = 0.05
TEMPERATURE = 0.1
ROUNDS = 3
LANES = 128
MESH = pl.DeviceIdType.MESH
F32 = jnp.float32
BF16 = jnp.bfloat16
NT = (((1,), (1,)), ((), ()))


def fold(x):
    return jnp.sum(x.reshape(x.shape[0] // 8, 8, LANES), axis=0)


def sums_kernel(
    n, protos, batch, queue,
    z1_hbm, z2_hbm, c_hbm, q1_hbm, q2_hbm,
    aall, pall, rinv, zt, cpad, small, lse_sum,
    xbuf, zall, sall, atr, cpart, csum,
    sem, recv_sem, zrecv_sem, xrecv_sem,
):
    tiles = cpad.shape[0] // LANES
    rows = batch + queue
    total_rows = n * rows
    coef = 1.0 / (2 * n * batch * TEMPERATURE)
    scale10 = math.log2(math.e) / TEMPERATURE
    scale20 = math.log2(math.e) / EPSILON

    me = lax.axis_index("data")
    bit0 = lax.rem(me, 2)
    bit1 = lax.rem(me // 2, 2)
    bit2 = me // 4
    chip = me // 2
    chips = n // 2
    odd = bit0 == 1
    even = bit0 == 0

    def peer(k):
        b0, b1, b2 = k % 2, (k // 2) % 2, k // 4
        return (lax.rem(bit2 + b2, 2) * 2 + lax.rem(bit1 + b1, 2)) * 2 + lax.rem(bit0 + b0, 2)

    far_first = (6, 7, 4, 5, 2, 3, 1)

    barrier = pltpu.get_barrier_semaphore()
    for k in far_first:
        pl.semaphore_signal(barrier, inc=1, device_id=(peer(k),), device_id_type=MESH)

    c_in = pltpu.make_async_copy(c_hbm, cpad.at[pl.ds(0, protos)], sem.at[2])

    def rows_in(v):
        z_hbm, q_hbm = ((z1_hbm, q1_hbm), (z2_hbm, q2_hbm))[v]
        pltpu.make_async_copy(z_hbm, xbuf.at[0, v, pl.ds(0, batch)], sem.at[v]).start()
        pltpu.make_async_copy(q_hbm, xbuf.at[0, v, pl.ds(batch, queue)], sem.at[v]).start()

    def wait_rows(v):
        pltpu.make_async_copy(xbuf.at[0, v], xbuf.at[0, v], sem.at[v]).wait()

    c_in.start()
    rows_in(0)
    rows_in(1)

    cpad[pl.ds(protos, cpad.shape[0] - protos), :] = jnp.zeros((cpad.shape[0] - protos, LANES), BF16)
    c_in.wait()

    lane = lax.broadcasted_iota(jnp.int32, (1, LANES), 1)
    tail_ok = lane < (protos - (tiles - 1) * LANES)
    tail_mask = tail_ok.astype(F32)

    def publish(t, v, acc, slot):
        for j in range(tiles):
            cpart[v, pl.ds(8 * j, 8), :] = acc[j]
        out = cpart[v, pl.ds(0, tiles, stride=8), :]
        for s in range(1, 8):
            out = out + cpart[v, pl.ds(s, tiles, stride=8), :]
        csum[t, v, slot] = out

    def sum_copy(t, v, k, slots):
        return pltpu.make_async_remote_copy(
            src_ref=csum.at[t, v, slots], dst_ref=csum.at[t, v, slots],
            send_sem=sem.at[v], recv_sem=recv_sem.at[t % 2, v],
            device_id=(peer(k),), device_id_type=MESH)

    def sums(t, v, count):
        return sum_copy(t, v, 1, pl.ds(0, count))

    def send_sums(t, v, slot, peers):
        for k in peers:
            sum_copy(t, v, k, slot).start()

    def col_scale(t, v, slots):
        c = csum[t, v, 0]
        for d in range(1, slots):
            c = c + csum[t, v, d]
        w = 1.0 / (protos * c)
        index = (lax.broadcasted_iota(jnp.int32, (tiles, LANES), 0) * LANES
                 + lax.broadcasted_iota(jnp.int32, (tiles, LANES), 1))
        small[v] = jnp.where(index < protos, w, 0.0)

    def first_pass(v, source, base):
        acc = [jnp.zeros((8, LANES), F32) for _ in range(tiles)]
        for start, size in ((0, rows // 2), (rows // 2, rows // 2)):
            x = xbuf[source, v, pl.ds(start, size), :]
            for jj in range(tiles // 2):
                s = lax.dot_general(x, cpad[pl.ds(jj * 256, 256), :], NT, preferred_element_type=F32)
                for h in range(2):
                    a = jnp.exp2(s[:, h * LANES:(h + 1) * LANES] * scale20)
                    atr[v, 2 * jj + h, pl.ds(base + start, size), :] = a
                    if base == 0:
                        acc[2 * jj + h] = acc[2 * jj + h] + fold(a)
        return acc

    def sink_pass(v):
        acc = [jnp.zeros((8, LANES), F32) for _ in range(tiles)]
        step = 128
        for b in range(2 * rows // step):
            sl = pl.ds(b * step, step)
            p = atr[v, 0, sl, :] * small[v, 0:1, :]
            for j in range(1, tiles):
                p = p + atr[v, j, sl, :] * small[v, j:j + 1, :]
            u = 1.0 / (total_rows * jnp.sum(p, axis=1, keepdims=True))
            for j in range(tiles):
                acc[j] = acc[j] + fold(atr[v, j, sl, :] * u)
        return acc

    def x_copy(v):
        return pltpu.make_async_remote_copy(
            src_ref=xbuf.at[0, v], dst_ref=xbuf.at[1, v], send_sem=sem.at[3], recv_sem=xrecv_sem.at[v],
            device_id=(peer(1),), device_id_type=MESH)

    def first_round(v):
        @pl.when(odd)
        def _():
            send_sums(0, v, me, (6, 4, 2))

        @pl.when(even)
        def _():
            send_sums(0, v, me, (7, 5, 3, 1))
            x_copy(v).start()

    wait_rows(0)
    publish(0, 0, first_pass(0, 0, 0), me)
    pl.semaphore_wait(barrier, n - 1)
    first_round(0)
    wait_rows(1)
    publish(0, 1, first_pass(1, 0, 0), me)
    first_round(1)

    def z_copy(k, target, src, dst):
        return pltpu.make_async_remote_copy(
            src_ref=src, dst_ref=dst, send_sem=sem.at[2], recv_sem=zrecv_sem.at[(0, 1, 2, 3)[k // 2] if k in (1, 2, 4, 6) else 4],
            device_id=(peer(target),), device_id_type=MESH)

    for k in (1, 2, 4, 6):
        for v in range(2):
            z_copy(k, k, xbuf.at[0, v, pl.ds(0, batch)], zall.at[me, v]).start()

    def z_arrived(k):
        z_copy(k, k, zall.at[peer(k)], zall.at[peer(k)]).wait_recv()

    def relays_arrived(k):
        z_copy(3, 1, zall.at[pl.ds(0, 3)], zall.at[pl.ds(0, 3)]).wait_recv()

    def relay(k):
        z_arrived(k)
        z_copy(k + 1, 1, zall.at[peer(k)], zall.at[peer(k)]).start()

    def block_of(k):
        return pl.ds(pl.multiple_of(peer(k) * batch, batch), batch)

    def transport(k):
        d = peer(k)
        z = [xbuf[0, v, pl.ds(0, batch), :] if k == 0 else zall[d, v] for v in range(2)]
        for v in range(2):
            zt[:, pl.ds(pl.multiple_of((v * n + d) * batch, batch), batch)] = z[v].astype(F32).T
        x = jnp.concatenate(z, axis=0)
        p = None
        for jj in range(tiles // 2):
            s = lax.dot_general(x, cpad[pl.ds(jj * 256, 256), :], NT, preferred_element_type=F32)
            for h in range(2):
                j = 2 * jj + h
                sj = s[:, h * LANES:(h + 1) * LANES]
                e = jnp.exp2(sj * scale10)
                if j == tiles - 1:
                    e = e * tail_mask
                a = e * e
                for v in range(2):
                    half = slice(v * batch, (v + 1) * batch)
                    aall[v, j, block_of(k), :] = a[half]
                    pall[v, j, block_of(k), :] = e[half]
                    sall[v, j, block_of(k), :] = sj[half]
                p = e if p is None else p + e
        return jnp.sum(p, axis=1, keepdims=True)

    def softmax(k, r):
        lse_sum[peer(k)] = fold(jnp.broadcast_to(jnp.log(r), (2 * batch, LANES)))
        inv = coef / r
        for v in range(2):
            for j in range(tiles):
                pall[v, j, block_of(k), :] = pall[v, j, block_of(k), :] * inv[v * batch:(v + 1) * batch]

    def prepare(steps):
        last = None
        for k, before in steps:
            before(k)
            r = transport(k)
            if last is not None:
                softmax(*last)
            last = k, r
        softmax(*last)

    def ready(k):
        pass

    @pl.when(odd)
    def _():
        prepare([(0, ready)])
        for v in range(2):
            x_copy(v).wait_recv()
            first_pass(v, 1, rows)
        for v in range(2):
            sums(0, v, n - 1).wait_recv()
            col_scale(0, v, n)
            sums(0, v, 3).wait_send()
            publish(1, v, sink_pass(v), chip)
            send_sums(1, v, chip, (6, 4, 2))
        prepare([(1, z_arrived), (2, relay), (4, relay)])
        relay(6)
        for v in range(2):
            sums(1, v, chips - 1).wait_recv()
            col_scale(1, v, chips)
            sums(1, v, chips - 1).wait_send()
            publish(2, v, sink_pass(v), chip)
            send_sums(2, v, chip, (7, 5, 3, 6, 4, 2, 1))
        prepare([(6, ready), (3, relays_arrived), (5, ready), (7, ready)])

    @pl.when(even)
    def _():
        prepare([(0, ready), (1, z_arrived), (2, relay), (4, relay)])
        relay(6)
        prepare([(6, ready), (3, relays_arrived), (5, ready), (7, ready)])

    def row_scale(v):
        w = [small[v, j:j + 1, :] for j in range(tiles)]

        def sums(d):
            sl = pl.ds(d * batch, batch)
            p = None
            m = None
            for j in range(tiles):
                t = aall[v, j, sl, :] * w[j]
                aall[v, j, sl, :] = t
                u = t * sall[1 - v, j, sl, :]
                p = t if p is None else p + t
                m = u if m is None else m + u
            return jnp.sum(p, axis=1, keepdims=True), m

        def scale(d, p, m):
            inv = 1.0 / p
            rinv[v, pl.ds(d * batch, batch), :] = jnp.broadcast_to(coef * inv, (batch, LANES))
            return fold(m * inv)

        part = jnp.zeros((8, LANES), F32)
        last = None
        for d in range(n):
            this = sums(d)
            if d > 0:
                part = part + scale(d - 1, *last)
            last = this
        return part + scale(n - 1, *last)

    def last_scale(v):
        @pl.when(odd)
        def _():
            sums(2, v, chips - 1).wait_recv()

        @pl.when(even)
        def _():
            sums(2, v, chips).wait_recv()

        col_scale(2, v, chips)

    last_scale(0)
    part = row_scale(0)
    last_scale(1)
    small[2] = part + row_scale(1)

    @pl.when(odd)
    def _():
        for v in range(2):
            sums(2, v, n - 1).wait_send()

    @pl.when(even)
    def _():
        for v in range(2):
            sums(0, v, 4).wait_send()
        pltpu.make_async_remote_copy(
            src_ref=xbuf.at[0], dst_ref=xbuf.at[1], send_sem=sem.at[3], recv_sem=xrecv_sem.at[0],
            device_id=(peer(1),), device_id_type=MESH).wait_send()

    z_copy(1, 1, zall.at[pl.ds(0, n - 1)], zall.at[pl.ds(0, n - 1)]).wait_send()


def grads_kernel(
    n, protos, batch,
    aall, pall, rinv, zt, cpad, small, lse_sum,
    codes1_hbm, codes2_hbm, loss_hbm, dz1_hbm, dz2_hbm, gp_hbm,
    codes, gp, dz, loss, out_sem,
):
    tiles = cpad.shape[0] // LANES
    batch_total = n * batch
    coef = 1.0 / (2 * batch_total * TEMPERATURE)
    me = lax.axis_index("data")
    own = pl.ds(pl.multiple_of(me * batch, batch), batch)
    codes_hbm = (codes1_hbm, codes2_hbm)
    dz_hbm = (dz1_hbm, dz2_hbm)

    logs = lse_sum[0]
    for d in range(1, n):
        logs = logs + lse_sum[d]
    total = jnp.sum(small[2]) * (1.0 / TEMPERATURE) - jnp.sum(logs) * (1.0 / LANES)
    loss[0, 0] = total * (-1.0 / (2 * batch_total))
    pltpu.make_async_copy(loss, loss_hbm, out_sem.at[5]).start()

    pairs = tiles // 2
    deep = 2 * batch

    def cols_of(jj):
        return pl.ds(jj * 2 * LANES, min(2 * LANES, protos - jj * 2 * LANES))

    def body(acc, dz_acc):
        for ref in (*acc[0], *acc[1], *dz_acc):
            pltpu.matmul_pop(ref)

        def tiles_of(big, v):
            for d in range(0, n, 2):
                sl = pl.ds(d * batch, deep)
                scale = rinv[v, sl, :]
                lhs = zt[:, pl.ds((1 - v) * n * batch + d * batch, deep)]
                reg = (d // 2) % 2
                for unit in range(2):
                    g = [pall[1 - v, j, sl, :] - aall[v, j, sl, :] * scale
                         for j in (4 * big + 2 * unit, 4 * big + 2 * unit + 1)]
                    pltpu.matmul_push_rhs(jnp.concatenate(g, axis=1), staging_register=reg, mxu_index=unit)
                    pltpu.matmul_acc_lhs(acc[big][unit], lhs, load_staged_rhs=reg)

        def own_part(jj):
            lhs = []
            for v in range(2):
                g = []
                for h in range(2):
                    j = 2 * jj + h
                    part = min(LANES, protos - j * LANES)
                    q = aall[v, j, own, :] * rinv[v, own, :]
                    g.append(pall[1 - v, j, own, :] - q)
                    codes[v, pl.ds(j * LANES, part), :] = (q * (1.0 / coef)).T[:part]
                lhs.insert(0, jnp.concatenate(g, axis=1))
            c = cpad[pl.ds(jj * 2 * LANES, 2 * LANES), :].astype(F32)
            pltpu.matmul_push_rhs(jnp.concatenate([c, c], axis=1), staging_register=0, mxu_index=jj % 2)
            pltpu.matmul_acc_lhs(dz_acc[jj % 2], jnp.concatenate(lhs, axis=0), load_staged_rhs=0)

        def drain(big):
            for unit in range(2):
                cols = cols_of(2 * big + unit)
                gp[cols, :] = pltpu.matmul_pop(acc[big][unit]).T[:cols.size]

        def send(big):
            for jj in (2 * big, 2 * big + 1):
                cols = cols_of(jj)
                pltpu.make_async_copy(gp.at[cols], gp_hbm.at[cols], out_sem.at[4]).start()

        def send_codes(big):
            for jj in (2 * big, 2 * big + 1):
                cols = cols_of(jj)
                for v in range(2):
                    pltpu.make_async_copy(codes.at[v, cols], codes_hbm[v].at[cols], out_sem.at[v]).start()

        own_part(0)
        own_part(1)
        send_codes(0)
        tiles_of(0, 0)
        tiles_of(0, 1)
        own_part(2)
        own_part(3)
        send_codes(1)
        tiles_of(1, 0)
        drain(0)
        send(0)
        o = pltpu.matmul_pop(dz_acc[0]) + pltpu.matmul_pop(dz_acc[1])
        for v in range(2):
            dz[v] = o[v * batch:(v + 1) * batch, :LANES]
            pltpu.make_async_copy(dz.at[v], dz_hbm[v], out_sem.at[2 + v]).start()
        tiles_of(1, 1)
        drain(1)
        send(1)

    def acc_of(rows):
        return tuple(pltpu.ACC(unit)((rows, 2 * LANES), F32) for unit in range(2))

    pl.run_scoped(body, (acc_of(LANES), acc_of(LANES)), acc_of(deep))

    for v in range(2):
        pltpu.make_async_copy(codes.at[v, pl.ds(0, protos)], codes_hbm[v], out_sem.at[v]).wait()
        pltpu.make_async_copy(dz.at[v], dz_hbm[v], out_sem.at[2 + v]).wait()
    pltpu.make_async_copy(gp.at[pl.ds(0, protos)], gp_hbm, out_sem.at[4]).wait()
    pltpu.make_async_copy(loss, loss_hbm, out_sem.at[5]).wait()


def solution(mesh):
    n = mesh.shape["data"]

    def local_step(z_one, z_two, protos, queue_one, queue_two):
        k, width = protos.shape
        batch, queue = z_one.shape[0], queue_one.shape[0]
        rows = batch + queue
        pad = (k + 255) // 256 * 256
        tiles = pad // LANES
        anywhere = pl.BlockSpec(memory_space=pl.ANY)
        sem = pltpu.SemaphoreType.DMA
        vmem = pl.BlockSpec(memory_space=pltpu.VMEM)
        whole = n * batch
        shared = pl.pallas_call(
            functools.partial(sums_kernel, n, k, batch, queue),
            out_shape=(
                pltpu.VMEM((2, tiles, whole, LANES), F32),
                pltpu.VMEM((2, tiles, whole, LANES), F32),
                pltpu.VMEM((2, whole, LANES), F32),
                pltpu.VMEM((width, 2 * whole), F32),
                pltpu.VMEM((pad, width), BF16),
                pltpu.VMEM((4, tiles, LANES), F32),
                pltpu.VMEM((n, 8, LANES), F32),
            ),
            in_specs=[anywhere] * 5,
            out_specs=(vmem,) * 7,
            scratch_shapes=[
                pltpu.VMEM((2, 2, rows, width), BF16),
                pltpu.VMEM((n, 2, batch, width), BF16),
                pltpu.VMEM((2, tiles, whole, LANES), F32),
                pltpu.VMEM((2, tiles, 2 * rows, LANES), F32),
                pltpu.VMEM((2, 8 * tiles, LANES), F32),
                pltpu.VMEM((ROUNDS, 2, n, tiles, LANES), F32),
                sem((4,)),
                sem((2, 2)),
                sem((5,)),
                sem((2,)),
            ],
            compiler_params=pltpu.CompilerParams(
                collective_id=0, has_side_effects=True, vmem_limit_bytes=26 << 20),
            name="sums",
        )(*(pltpu.with_memory_space_constraint(x, pltpu.HBM) for x in (z_one, z_two, protos, queue_one, queue_two)))
        codes_one, codes_two, loss, dz_one, dz_two, grad_protos = pl.pallas_call(
            functools.partial(grads_kernel, n, k, batch),
            out_shape=(
                jax.ShapeDtypeStruct((k, batch), F32),
                jax.ShapeDtypeStruct((k, batch), F32),
                jax.ShapeDtypeStruct((1, 1), F32),
                jax.ShapeDtypeStruct((batch, width), F32),
                jax.ShapeDtypeStruct((batch, width), F32),
                jax.ShapeDtypeStruct((k, width), F32),
            ),
            in_specs=[vmem] * 7,
            out_specs=(anywhere,) * 6,
            scratch_shapes=[
                pltpu.VMEM((2, pad, batch), F32),
                pltpu.VMEM((pad, width), F32),
                pltpu.VMEM((2, batch, width), F32),
                pltpu.SMEM((1, 1), F32),
                sem((6,)),
            ],
            compiler_params=pltpu.CompilerParams(vmem_limit_bytes=14 << 20),
            name="grads",
        )(*shared)
        return codes_one.T, codes_two.T, loss[0, 0], dz_one, dz_two, grad_protos

    row_spec = P("data", None)
    full_spec = P(None, None)
    return jax.shard_map(
        local_step,
        mesh=mesh,
        in_specs=(row_spec, row_spec, full_spec, row_spec, row_spec),
        out_specs=(row_spec, row_spec, P(), row_spec, row_spec, full_spec),
        check_vma=False,
    )
```

```python
import functools
import math

import jax
import jax.numpy as jnp
from jax import lax
from jax.experimental import pallas as pl
from jax.experimental.pallas import tpu as pltpu
from jax.sharding import PartitionSpec as P

EPSILON = 0.05
TEMPERATURE = 0.1
ROUNDS = 3
LANES = 128
MESH = pl.DeviceIdType.MESH
F32 = jnp.float32
BF16 = jnp.bfloat16
NT = (((1,), (1,)), ((), ()))


def fold(x):
    return jnp.sum(x.reshape(x.shape[0] // 8, 8, LANES), axis=0)


def sums_kernel(
    n, protos, batch, queue,
    z1_hbm, z2_hbm, c_hbm, q1_hbm, q2_hbm,
    aall, pall, rinv, zt, cpad, small, lse_sum,
    xbuf, zall, sall, atr, cpart, csum,
    sem, recv_sem, zrecv_sem, xrecv_sem,
):
    tiles = cpad.shape[0] // LANES
    rows = batch + queue
    total_rows = n * rows
    coef = 1.0 / (2 * n * batch * TEMPERATURE)
    scale10 = math.log2(math.e) / TEMPERATURE
    scale20 = math.log2(math.e) / EPSILON

    me = lax.axis_index("data")
    bit0 = lax.rem(me, 2)
    bit1 = lax.rem(me // 2, 2)
    bit2 = me // 4
    chip = me // 2
    chips = n // 2
    odd = bit0 == 1
    even = bit0 == 0

    def peer(k):
        b0, b1, b2 = k % 2, (k // 2) % 2, k // 4
        return (lax.rem(bit2 + b2, 2) * 2 + lax.rem(bit1 + b1, 2)) * 2 + lax.rem(bit0 + b0, 2)

    far_first = (6, 7, 4, 5, 2, 3, 1)

    barrier = pltpu.get_barrier_semaphore()
    c_in = pltpu.make_async_copy(c_hbm, cpad.at[pl.ds(0, protos)], sem.at[2])

    def rows_in(v):
        z_hbm, q_hbm = ((z1_hbm, q1_hbm), (z2_hbm, q2_hbm))[v]
        pltpu.make_async_copy(z_hbm, xbuf.at[0, v, pl.ds(0, batch)], sem.at[v]).start()
        pltpu.make_async_copy(q_hbm, xbuf.at[0, v, pl.ds(batch, queue)], sem.at[v]).start()

    def wait_rows(v):
        pltpu.make_async_copy(xbuf.at[0, v], xbuf.at[0, v], sem.at[v]).wait()

    c_in.start()
    rows_in(0)
    for k in far_first:
        pl.semaphore_signal(barrier, inc=1, device_id=(peer(k),), device_id_type=MESH)
    rows_in(1)

    cpad[pl.ds(protos, cpad.shape[0] - protos), :] = jnp.zeros((cpad.shape[0] - protos, LANES), BF16)
    c_in.wait()

    lane = lax.broadcasted_iota(jnp.int32, (1, LANES), 1)
    tail_ok = lane < (protos - (tiles - 1) * LANES)
    tail_mask = tail_ok.astype(F32)

    def publish(t, v, acc, slot):
        for j in range(tiles):
            cpart[v, pl.ds(8 * j, 8), :] = acc[j]
        out = cpart[v, pl.ds(0, tiles, stride=8), :]
        for s in range(1, 8):
            out = out + cpart[v, pl.ds(s, tiles, stride=8), :]
        csum[t, v, slot] = out

    def sum_copy(t, v, k, slots):
        return pltpu.make_async_remote_copy(
            src_ref=csum.at[t, v, slots], dst_ref=csum.at[t, v, slots],
            send_sem=sem.at[v], recv_sem=recv_sem.at[t % 2, v],
            device_id=(peer(k),), device_id_type=MESH)

    def sums(t, v, count):
        return sum_copy(t, v, 1, pl.ds(0, count))

    def send_sums(t, v, slot, peers):
        for k in peers:
            sum_copy(t, v, k, slot).start()

    def col_scale(t, v, slots):
        c = csum[t, v, 0]
        for d in range(1, slots):
            c = c + csum[t, v, d]
        w = 1.0 / (protos * c)
        index = (lax.broadcasted_iota(jnp.int32, (tiles, LANES), 0) * LANES
                 + lax.broadcasted_iota(jnp.int32, (tiles, LANES), 1))
        small[v] = jnp.where(index < protos, w, 0.0)

    def first_pass(v, source, base):
        acc = [jnp.zeros((8, LANES), F32) for _ in range(tiles)]
        for start, size in ((0, rows // 2), (rows // 2, rows // 2)):
            x = xbuf[source, v, pl.ds(start, size), :]
            for jj in range(tiles // 2):
                s = lax.dot_general(x, cpad[pl.ds(jj * 256, 256), :], NT, preferred_element_type=F32)
                for h in range(2):
                    a = jnp.exp2(s[:, h * LANES:(h + 1) * LANES] * scale20)
                    atr[v, 2 * jj + h, pl.ds(base + start, size), :] = a
                    if base == 0:
                        acc[2 * jj + h] = acc[2 * jj + h] + fold(a)
        return acc

    def sink_pass(v):
        acc = [jnp.zeros((8, LANES), F32) for _ in range(tiles)]
        step = 128
        for b in range(2 * rows // step):
            sl = pl.ds(b * step, step)
            p = atr[v, 0, sl, :] * small[v, 0:1, :]
            for j in range(1, tiles):
                p = p + atr[v, j, sl, :] * small[v, j:j + 1, :]
            u = 1.0 / (total_rows * jnp.sum(p, axis=1, keepdims=True))
            for j in range(tiles):
                acc[j] = acc[j] + fold(atr[v, j, sl, :] * u)
        return acc

    def x_copy(v):
        return pltpu.make_async_remote_copy(
            src_ref=xbuf.at[0, v], dst_ref=xbuf.at[1, v], send_sem=sem.at[3], recv_sem=xrecv_sem.at[v],
            device_id=(peer(1),), device_id_type=MESH)

    def first_round(v):
        @pl.when(odd)
        def _():
            send_sums(0, v, me, (6, 4, 2))

        @pl.when(even)
        def _():
            send_sums(0, v, me, (7, 5, 3, 1))
            x_copy(v).start()

    wait_rows(0)
    publish(0, 0, first_pass(0, 0, 0), me)
    pl.semaphore_wait(barrier, n - 1)
    first_round(0)
    wait_rows(1)
    publish(0, 1, first_pass(1, 0, 0), me)
    first_round(1)

    def z_copy(k, target, src, dst):
        return pltpu.make_async_remote_copy(
            src_ref=src, dst_ref=dst, send_sem=sem.at[2], recv_sem=zrecv_sem.at[(0, 0, 1, 4, 2, 4, 3, 3)[k]],
            device_id=(peer(target),), device_id_type=MESH)

    def z_send(k):
        for v in range(2):
            z_copy(k, k, xbuf.at[0, v, pl.ds(0, batch)], zall.at[me, v]).start()

    def z_pass(k, owner, target):
        z_copy(k, target, zall.at[peer(owner)], zall.at[peer(owner)]).start()

    def z_arrived(k, count=1):
        z_copy(k, 1, zall.at[pl.ds(0, count)], zall.at[pl.ds(0, count)]).wait_recv()

    def relay(k):
        z_arrived(k)
        z_pass(k + 1, k, 1)

    def to_diagonal(k):
        z_arrived(k)
        z_pass(7, 1, 6)

    def relay_diagonal(k):
        z_arrived(6, 2)
        z_pass(7, 6, 1)
        z_pass(6, 7, 1)

    def side_arrived(k):
        z_arrived(3, 2)

    def diagonal_arrived(k):
        z_arrived(6, 2)

    for k in (1, 2, 4):
        z_send(k)

    @pl.when(even)
    def _():
        z_send(6)

    def block_of(k):
        return pl.ds(pl.multiple_of(peer(k) * batch, batch), batch)

    def transport(k):
        d = peer(k)
        z = [xbuf[0, v, pl.ds(0, batch), :] if k == 0 else zall[d, v] for v in range(2)]
        for v in range(2):
            zt[:, pl.ds(pl.multiple_of((v * n + d) * batch, batch), batch)] = z[v].astype(F32).T
        x = jnp.concatenate(z, axis=0)
        p = None
        for jj in range(tiles // 2):
            s = lax.dot_general(x, cpad[pl.ds(jj * 256, 256), :], NT, preferred_element_type=F32)
            for h in range(2):
                j = 2 * jj + h
                sj = s[:, h * LANES:(h + 1) * LANES]
                e = jnp.exp2(sj * scale10)
                if j == tiles - 1:
                    e = e * tail_mask
                a = e * e
                for v in range(2):
                    half = slice(v * batch, (v + 1) * batch)
                    aall[v, j, block_of(k), :] = a[half]
                    pall[v, j, block_of(k), :] = e[half]
                    sall[v, j, block_of(k), :] = sj[half]
                p = e if p is None else p + e
        return jnp.sum(p, axis=1, keepdims=True)

    def softmax(k, r):
        lse_sum[peer(k)] = fold(jnp.broadcast_to(jnp.log(r), (2 * batch, LANES)))
        inv = coef / r
        for v in range(2):
            for j in range(tiles):
                pall[v, j, block_of(k), :] = pall[v, j, block_of(k), :] * inv[v * batch:(v + 1) * batch]

    def prepare(steps):
        last = None
        for k, before in steps:
            before(k)
            r = transport(k)
            if last is not None:
                softmax(*last)
            last = k, r
        softmax(*last)

    def ready(k):
        pass

    @pl.when(odd)
    def _():
        prepare([(0, ready)])
        for v in range(2):
            x_copy(v).wait_recv()
            first_pass(v, 1, rows)
        for v in range(2):
            sums(0, v, n - 1).wait_recv()
            col_scale(0, v, n)
            sums(0, v, 3).wait_send()
            publish(1, v, sink_pass(v), chip)
            send_sums(1, v, chip, (6, 4, 2))
        prepare([(1, z_arrived), (2, relay), (4, relay)])
        for v in range(2):
            sums(1, v, chips - 1).wait_recv()
            col_scale(1, v, chips)
            sums(1, v, chips - 1).wait_send()
            publish(2, v, sink_pass(v), chip)
            send_sums(2, v, chip, (7, 5, 3, 6, 4, 2, 1))
        prepare([(3, side_arrived), (5, ready), (6, diagonal_arrived), (7, ready)])

    @pl.when(even)
    def _():
        prepare([(0, ready), (1, to_diagonal), (2, relay), (4, relay)])
        prepare([(6, relay_diagonal), (7, ready), (3, side_arrived), (5, ready)])

    def row_scale(v):
        w = [small[v, j:j + 1, :] for j in range(tiles)]

        def sums(d):
            sl = pl.ds(d * batch, batch)
            p = None
            m = None
            for j in range(tiles):
                t = aall[v, j, sl, :] * w[j]
                aall[v, j, sl, :] = t
                u = t * sall[1 - v, j, sl, :]
                p = t if p is None else p + t
                m = u if m is None else m + u
            return jnp.sum(p, axis=1, keepdims=True), m

        def scale(d, p, m):
            inv = 1.0 / p
            rinv[v, pl.ds(d * batch, batch), :] = jnp.broadcast_to(coef * inv, (batch, LANES))
            return fold(m * inv)

        part = jnp.zeros((8, LANES), F32)
        last = None
        for d in range(n):
            this = sums(d)
            if d > 0:
                part = part + scale(d - 1, *last)
            last = this
        return part + scale(n - 1, *last)

    def last_scale(v):
        @pl.when(odd)
        def _():
            sums(2, v, chips - 1).wait_recv()

        @pl.when(even)
        def _():
            sums(2, v, chips).wait_recv()

        col_scale(2, v, chips)

    def z_sent(count):
        z_copy(1, 1, zall.at[pl.ds(0, count)], zall.at[pl.ds(0, count)]).wait_send()

    last_scale(0)
    part = row_scale(0)
    last_scale(1)
    small[2] = part + row_scale(1)

    @pl.when(odd)
    def _():
        for v in range(2):
            sums(2, v, n - 1).wait_send()
        z_sent(5)

    @pl.when(even)
    def _():
        for v in range(2):
            sums(0, v, 4).wait_send()
        pltpu.make_async_remote_copy(
            src_ref=xbuf.at[0], dst_ref=xbuf.at[1], send_sem=sem.at[3], recv_sem=xrecv_sem.at[0],
            device_id=(peer(1),), device_id_type=MESH).wait_send()
        z_sent(n)
        z_sent(1)


def grads_kernel(
    n, protos, batch,
    aall, pall, rinv, zt, cpad, small, lse_sum,
    codes1_hbm, codes2_hbm, loss_hbm, dz1_hbm, dz2_hbm, gp_hbm,
    codes, gp, dz, loss, out_sem,
):
    tiles = cpad.shape[0] // LANES
    batch_total = n * batch
    coef = 1.0 / (2 * batch_total * TEMPERATURE)
    me = lax.axis_index("data")
    own = pl.ds(pl.multiple_of(me * batch, batch), batch)
    codes_hbm = (codes1_hbm, codes2_hbm)
    dz_hbm = (dz1_hbm, dz2_hbm)

    logs = lse_sum[0]
    for d in range(1, n):
        logs = logs + lse_sum[d]
    total = jnp.sum(small[2]) * (1.0 / TEMPERATURE) - jnp.sum(logs) * (1.0 / LANES)
    loss[0, 0] = total * (-1.0 / (2 * batch_total))
    pltpu.make_async_copy(loss, loss_hbm, out_sem.at[5]).start()

    pairs = tiles // 2
    deep = 2 * batch

    def cols_of(jj):
        return pl.ds(jj * 2 * LANES, min(2 * LANES, protos - jj * 2 * LANES))

    def body(acc, dz_acc):
        for ref in (*acc[0], *acc[1], *dz_acc):
            pltpu.matmul_pop(ref)

        def tiles_of(big, v):
            for d in range(0, n, 2):
                sl = pl.ds(d * batch, deep)
                scale = rinv[v, sl, :]
                lhs = zt[:, pl.ds((1 - v) * n * batch + d * batch, deep)]
                reg = (d // 2) % 2
                for unit in range(2):
                    g = [pall[1 - v, j, sl, :] - aall[v, j, sl, :] * scale
                         for j in (4 * big + 2 * unit, 4 * big + 2 * unit + 1)]
                    pltpu.matmul_push_rhs(jnp.concatenate(g, axis=1), staging_register=reg, mxu_index=unit)
                    pltpu.matmul_acc_lhs(acc[big][unit], lhs, load_staged_rhs=reg)

        def own_part(jj):
            lhs = []
            for v in range(2):
                g = []
                for h in range(2):
                    j = 2 * jj + h
                    part = min(LANES, protos - j * LANES)
                    q = aall[v, j, own, :] * rinv[v, own, :]
                    g.append(pall[1 - v, j, own, :] - q)
                    codes[v, pl.ds(j * LANES, part), :] = (q * (1.0 / coef)).T[:part]
                lhs.insert(0, jnp.concatenate(g, axis=1))
            c = cpad[pl.ds(jj * 2 * LANES, 2 * LANES), :].astype(F32)
            pltpu.matmul_push_rhs(jnp.concatenate([c, c], axis=1), staging_register=0, mxu_index=jj % 2)
            pltpu.matmul_acc_lhs(dz_acc[jj % 2], jnp.concatenate(lhs, axis=0), load_staged_rhs=0)

        def drain(big):
            for unit in range(2):
                cols = cols_of(2 * big + unit)
                gp[cols, :] = pltpu.matmul_pop(acc[big][unit]).T[:cols.size]

        def send(big):
            for jj in (2 * big, 2 * big + 1):
                cols = cols_of(jj)
                pltpu.make_async_copy(gp.at[cols], gp_hbm.at[cols], out_sem.at[4]).start()

        def send_codes(big):
            for jj in (2 * big, 2 * big + 1):
                cols = cols_of(jj)
                for v in range(2):
                    pltpu.make_async_copy(codes.at[v, cols], codes_hbm[v].at[cols], out_sem.at[v]).start()

        own_part(0)
        own_part(1)
        send_codes(0)
        tiles_of(0, 0)
        tiles_of(0, 1)
        own_part(2)
        own_part(3)
        send_codes(1)
        tiles_of(1, 0)
        drain(0)
        send(0)
        o = pltpu.matmul_pop(dz_acc[0]) + pltpu.matmul_pop(dz_acc[1])
        for v in range(2):
            dz[v] = o[v * batch:(v + 1) * batch, :LANES]
            pltpu.make_async_copy(dz.at[v], dz_hbm[v], out_sem.at[2 + v]).start()
        tiles_of(1, 1)
        drain(1)
        send(1)

    def acc_of(rows):
        return tuple(pltpu.ACC(unit)((rows, 2 * LANES), F32) for unit in range(2))

    pl.run_scoped(body, (acc_of(LANES), acc_of(LANES)), acc_of(deep))

    for v in range(2):
        pltpu.make_async_copy(codes.at[v, pl.ds(0, protos)], codes_hbm[v], out_sem.at[v]).wait()
        pltpu.make_async_copy(dz.at[v], dz_hbm[v], out_sem.at[2 + v]).wait()
    pltpu.make_async_copy(gp.at[pl.ds(0, protos)], gp_hbm, out_sem.at[4]).wait()
    pltpu.make_async_copy(loss, loss_hbm, out_sem.at[5]).wait()


def solution(mesh):
    n = mesh.shape["data"]

    def local_step(z_one, z_two, protos, queue_one, queue_two):
        k, width = protos.shape
        batch, queue = z_one.shape[0], queue_one.shape[0]
        rows = batch + queue
        pad = (k + 255) // 256 * 256
        tiles = pad // LANES
        anywhere = pl.BlockSpec(memory_space=pl.ANY)
        sem = pltpu.SemaphoreType.DMA
        vmem = pl.BlockSpec(memory_space=pltpu.VMEM)
        whole = n * batch
        shared = pl.pallas_call(
            functools.partial(sums_kernel, n, k, batch, queue),
            out_shape=(
                pltpu.VMEM((2, tiles, whole, LANES), F32),
                pltpu.VMEM((2, tiles, whole, LANES), F32),
                pltpu.VMEM((2, whole, LANES), F32),
                pltpu.VMEM((width, 2 * whole), F32),
                pltpu.VMEM((pad, width), BF16),
                pltpu.VMEM((4, tiles, LANES), F32),
                pltpu.VMEM((n, 8, LANES), F32),
            ),
            in_specs=[anywhere] * 5,
            out_specs=(vmem,) * 7,
            scratch_shapes=[
                pltpu.VMEM((2, 2, rows, width), BF16),
                pltpu.VMEM((n, 2, batch, width), BF16),
                pltpu.VMEM((2, tiles, whole, LANES), F32),
                pltpu.VMEM((2, tiles, 2 * rows, LANES), F32),
                pltpu.VMEM((2, 8 * tiles, LANES), F32),
                pltpu.VMEM((ROUNDS, 2, n, tiles, LANES), F32),
                sem((4,)),
                sem((2, 2)),
                sem((5,)),
                sem((2,)),
            ],
            compiler_params=pltpu.CompilerParams(
                collective_id=0, has_side_effects=True, vmem_limit_bytes=26 << 20),
            name="sums",
        )(*(pltpu.with_memory_space_constraint(x, pltpu.HBM) for x in (z_one, z_two, protos, queue_one, queue_two)))
        codes_one, codes_two, loss, dz_one, dz_two, grad_protos = pl.pallas_call(
            functools.partial(grads_kernel, n, k, batch),
            out_shape=(
                jax.ShapeDtypeStruct((k, batch), F32),
                jax.ShapeDtypeStruct((k, batch), F32),
                jax.ShapeDtypeStruct((1, 1), F32),
                jax.ShapeDtypeStruct((batch, width), F32),
                jax.ShapeDtypeStruct((batch, width), F32),
                jax.ShapeDtypeStruct((k, width), F32),
            ),
            in_specs=[vmem] * 7,
            out_specs=(anywhere,) * 6,
            scratch_shapes=[
                pltpu.VMEM((2, pad, batch), F32),
                pltpu.VMEM((pad, width), F32),
                pltpu.VMEM((2, batch, width), F32),
                pltpu.SMEM((1, 1), F32),
                sem((6,)),
            ],
            compiler_params=pltpu.CompilerParams(vmem_limit_bytes=14 << 20),
            name="grads",
        )(*shared)
        return codes_one.T, codes_two.T, loss[0, 0], dz_one, dz_two, grad_protos

    row_spec = P("data", None)
    full_spec = P(None, None)
    return jax.shard_map(
        local_step,
        mesh=mesh,
        in_specs=(row_spec, row_spec, full_spec, row_spec, row_spec),
        out_specs=(row_spec, row_spec, P(), row_spec, row_spec, full_spec),
        check_vma=False,
    )
```

```python
import functools
import math

import jax
import jax.numpy as jnp
from jax import lax
from jax.experimental import pallas as pl
from jax.experimental.pallas import tpu as pltpu
from jax.sharding import PartitionSpec as P

EPSILON = 0.05
TEMPERATURE = 0.1
ROUNDS = 3
LANES = 128
MESH = pl.DeviceIdType.MESH
F32 = jnp.float32
BF16 = jnp.bfloat16
NT = (((1,), (1,)), ((), ()))


def fold(x):
    return jnp.sum(x.reshape(x.shape[0] // 8, 8, LANES), axis=0)


def sums_kernel(
    n, protos, batch, queue,
    z1_hbm, z2_hbm, c_hbm, q1_hbm, q2_hbm,
    aall, pall, rinv, zt, cpad, small, lse_sum,
    xbuf, zall, sall, atr, cpart, csum,
    sem, recv_sem, zrecv_sem, xrecv_sem,
):
    tiles = cpad.shape[0] // LANES
    rows = batch + queue
    total_rows = n * rows
    coef = 1.0 / (2 * n * batch * TEMPERATURE)
    scale10 = math.log2(math.e) / TEMPERATURE
    scale20 = math.log2(math.e) / EPSILON

    me = lax.axis_index("data")
    bit0 = lax.rem(me, 2)
    bit1 = lax.rem(me // 2, 2)
    bit2 = me // 4
    chip = me // 2
    chips = n // 2
    odd = bit0 == 1
    even = bit0 == 0

    def peer(k):
        b0, b1, b2 = k % 2, (k // 2) % 2, k // 4
        return (lax.rem(bit2 + b2, 2) * 2 + lax.rem(bit1 + b1, 2)) * 2 + lax.rem(bit0 + b0, 2)

    far_first = (6, 7, 4, 5, 2, 3, 1)

    barrier = pltpu.get_barrier_semaphore()
    c_in = pltpu.make_async_copy(c_hbm, cpad.at[pl.ds(0, protos)], sem.at[2])

    def rows_in(v):
        z_hbm, q_hbm = ((z1_hbm, q1_hbm), (z2_hbm, q2_hbm))[v]
        pltpu.make_async_copy(z_hbm, xbuf.at[0, v, pl.ds(0, batch)], sem.at[v]).start()
        pltpu.make_async_copy(q_hbm, xbuf.at[0, v, pl.ds(batch, queue)], sem.at[v]).start()

    def wait_rows(v):
        pltpu.make_async_copy(xbuf.at[0, v], xbuf.at[0, v], sem.at[v]).wait()

    c_in.start()
    rows_in(0)
    for k in far_first:
        pl.semaphore_signal(barrier, inc=1, device_id=(peer(k),), device_id_type=MESH)
    rows_in(1)

    cpad[pl.ds(protos, cpad.shape[0] - protos), :] = jnp.zeros((cpad.shape[0] - protos, LANES), BF16)
    c_in.wait()

    lane = lax.broadcasted_iota(jnp.int32, (1, LANES), 1)
    tail_ok = lane < (protos - (tiles - 1) * LANES)
    tail_mask = tail_ok.astype(F32)

    def publish(t, v, acc, slot):
        for j in range(tiles):
            cpart[v, pl.ds(8 * j, 8), :] = acc[j]
        out = cpart[v, pl.ds(0, tiles, stride=8), :]
        for s in range(1, 8):
            out = out + cpart[v, pl.ds(s, tiles, stride=8), :]
        csum[t, v, slot] = out

    def sum_copy(t, v, k, slots):
        return pltpu.make_async_remote_copy(
            src_ref=csum.at[t, v, slots], dst_ref=csum.at[t, v, slots],
            send_sem=sem.at[v], recv_sem=recv_sem.at[t % 2, v],
            device_id=(peer(k),), device_id_type=MESH)

    def sums(t, v, count):
        return sum_copy(t, v, 1, pl.ds(0, count))

    def send_sums(t, v, slot, peers):
        for k in peers:
            sum_copy(t, v, k, slot).start()

    def col_scale(t, v, slots):
        c = csum[t, v, 0]
        for d in range(1, slots):
            c = c + csum[t, v, d]
        w = 1.0 / (protos * c)
        index = (lax.broadcasted_iota(jnp.int32, (tiles, LANES), 0) * LANES
                 + lax.broadcasted_iota(jnp.int32, (tiles, LANES), 1))
        small[v] = jnp.where(index < protos, w, 0.0)

    def first_pass(v, source, base):
        acc = [jnp.zeros((8, LANES), F32) for _ in range(tiles)]
        for start, size in ((0, rows // 2), (rows // 2, rows // 2)):
            x = xbuf[source, v, pl.ds(start, size), :]
            for jj in range(tiles // 2):
                s = lax.dot_general(x, cpad[pl.ds(jj * 256, 256), :], NT, preferred_element_type=F32)
                for h in range(2):
                    a = jnp.exp2(s[:, h * LANES:(h + 1) * LANES] * scale20)
                    atr[v, 2 * jj + h, pl.ds(base + start, size), :] = a
                    if base == 0:
                        acc[2 * jj + h] = acc[2 * jj + h] + fold(a)
        return acc

    def sink_pass(v):
        acc = [jnp.zeros((8, LANES), F32) for _ in range(tiles)]
        step = 128
        for b in range(2 * rows // step):
            sl = pl.ds(b * step, step)
            p = atr[v, 0, sl, :] * small[v, 0:1, :]
            for j in range(1, tiles):
                p = p + atr[v, j, sl, :] * small[v, j:j + 1, :]
            u = 1.0 / (total_rows * jnp.sum(p, axis=1, keepdims=True))
            for j in range(tiles):
                acc[j] = acc[j] + fold(atr[v, j, sl, :] * u)
        return acc

    def x_copy(v):
        return pltpu.make_async_remote_copy(
            src_ref=xbuf.at[0, v], dst_ref=xbuf.at[1, v], send_sem=sem.at[3], recv_sem=xrecv_sem.at[v],
            device_id=(peer(1),), device_id_type=MESH)

    def first_round(v):
        @pl.when(odd)
        def _():
            send_sums(0, v, me, (6, 4, 2))

        @pl.when(even)
        def _():
            send_sums(0, v, me, (7, 5, 3, 1))
            x_copy(v).start()

    wait_rows(0)
    publish(0, 0, first_pass(0, 0, 0), me)
    pl.semaphore_wait(barrier, n - 1)
    first_round(0)
    wait_rows(1)
    publish(0, 1, first_pass(1, 0, 0), me)
    first_round(1)

    def z_copy(k, target, src, dst):
        return pltpu.make_async_remote_copy(
            src_ref=src, dst_ref=dst, send_sem=sem.at[2], recv_sem=zrecv_sem.at[(0, 0, 1, 4, 2, 4, 3, 3)[k]],
            device_id=(peer(target),), device_id_type=MESH)

    def z_send(k):
        for v in range(2):
            z_copy(k, k, xbuf.at[0, v, pl.ds(0, batch)], zall.at[me, v]).start()

    def z_pass(k, owner, target):
        z_copy(k, target, zall.at[peer(owner)], zall.at[peer(owner)]).start()

    def z_arrived(k, count=1):
        z_copy(k, 1, zall.at[pl.ds(0, count)], zall.at[pl.ds(0, count)]).wait_recv()

    def relay(k):
        z_arrived(k)
        z_pass(k + 1, k, 1)

    def to_diagonal(k):
        z_arrived(k)
        z_pass(7, 1, 6)

    def relay_diagonal(k):
        z_arrived(6, 2)
        z_pass(7, 6, 1)
        z_pass(6, 7, 1)

    def side_arrived(k):
        z_arrived(3, 2)

    def diagonal_arrived(k):
        z_arrived(6, 2)

    for k in (1, 2, 4):
        z_send(k)

    @pl.when(even)
    def _():
        z_send(6)

    def block_of(k):
        return pl.ds(pl.multiple_of(peer(k) * batch, batch), batch)

    def transport(k):
        d = peer(k)
        z = [xbuf[0, v, pl.ds(0, batch), :] if k == 0 else zall[d, v] for v in range(2)]
        for v in range(2):
            zt[:, pl.ds(pl.multiple_of((v * n + d) * batch, batch), batch)] = z[v].astype(F32).T
        x = jnp.concatenate(z, axis=0)
        p = None
        for jj in range(tiles // 2):
            s = lax.dot_general(x, cpad[pl.ds(jj * 256, 256), :], NT, preferred_element_type=F32)
            for h in range(2):
                j = 2 * jj + h
                sj = s[:, h * LANES:(h + 1) * LANES]
                e = jnp.exp2(sj * scale10)
                if j == tiles - 1:
                    e = e * tail_mask
                a = e * e
                for v in range(2):
                    half = slice(v * batch, (v + 1) * batch)
                    aall[v, j, block_of(k), :] = a[half]
                    pall[v, j, block_of(k), :] = e[half]
                    sall[v, j, block_of(k), :] = sj[half]
                p = e if p is None else p + e
        return jnp.sum(p, axis=1, keepdims=True)

    def softmax(k, r):
        lse_sum[peer(k)] = fold(jnp.broadcast_to(jnp.log(r), (2 * batch, LANES)))
        inv = coef / r
        for v in range(2):
            for j in range(tiles):
                pall[v, j, block_of(k), :] = pall[v, j, block_of(k), :] * inv[v * batch:(v + 1) * batch]

    def prepare(steps):
        last = None
        for k, before in steps:
            before(k)
            r = transport(k)
            if last is not None:
                softmax(*last)
            last = k, r
        softmax(*last)

    def ready(k):
        pass

    @pl.when(odd)
    def _():
        prepare([(0, ready)])
        for v in range(2):
            x_copy(v).wait_recv()
            first_pass(v, 1, rows)
        for v in range(2):
            sums(0, v, n - 1).wait_recv()
            col_scale(0, v, n)
            sums(0, v, 3).wait_send()
            publish(1, v, sink_pass(v), chip)
            send_sums(1, v, chip, (6, 4, 2))
        prepare([(1, z_arrived), (2, relay), (4, relay)])
        for v in range(2):
            sums(1, v, chips - 1).wait_recv()
            col_scale(1, v, chips)
            sums(1, v, chips - 1).wait_send()
            publish(2, v, sink_pass(v), chip)
            send_sums(2, v, chip, (7, 5, 3, 6, 4, 2, 1))
        prepare([(3, side_arrived), (5, ready), (6, diagonal_arrived), (7, ready)])

    @pl.when(even)
    def _():
        prepare([(0, ready), (1, to_diagonal), (2, relay), (4, relay)])
        prepare([(6, relay_diagonal), (7, ready), (3, side_arrived), (5, ready)])

    def row_scale(v):
        w = [small[v, j:j + 1, :] for j in range(tiles)]

        def sums(d):
            sl = pl.ds(d * batch, batch)
            p = None
            m = None
            for j in range(tiles):
                t = aall[v, j, sl, :] * w[j]
                if v == 0:
                    aall[v, j, sl, :] = t
                u = t * sall[1 - v, j, sl, :]
                p = t if p is None else p + t
                m = u if m is None else m + u
            return jnp.sum(p, axis=1, keepdims=True), m

        def scale(d, p, m):
            inv = 1.0 / p
            rinv[v, pl.ds(d * batch, batch), :] = jnp.broadcast_to(coef * inv, (batch, LANES))
            return fold(m * inv)

        part = jnp.zeros((8, LANES), F32)
        last = None
        for d in range(n):
            this = sums(d)
            if d > 0:
                part = part + scale(d - 1, *last)
            last = this
        return part + scale(n - 1, *last)

    def last_scale(v):
        @pl.when(odd)
        def _():
            sums(2, v, chips - 1).wait_recv()

        @pl.when(even)
        def _():
            sums(2, v, chips).wait_recv()

        col_scale(2, v, chips)

    def z_sent(count):
        z_copy(1, 1, zall.at[pl.ds(0, count)], zall.at[pl.ds(0, count)]).wait_send()

    last_scale(0)
    part = row_scale(0)
    last_scale(1)
    small[2] = part + row_scale(1)

    @pl.when(odd)
    def _():
        for v in range(2):
            sums(2, v, n - 1).wait_send()
        z_sent(5)

    @pl.when(even)
    def _():
        for v in range(2):
            sums(0, v, 4).wait_send()
        pltpu.make_async_remote_copy(
            src_ref=xbuf.at[0], dst_ref=xbuf.at[1], send_sem=sem.at[3], recv_sem=xrecv_sem.at[0],
            device_id=(peer(1),), device_id_type=MESH).wait_send()
        z_sent(n)
        z_sent(1)


def grads_kernel(
    n, protos, batch,
    aall, pall, rinv, zt, cpad, small, lse_sum,
    codes1_hbm, codes2_hbm, loss_hbm, dz1_hbm, dz2_hbm, gp_hbm,
    codes, gp, dz, loss, out_sem,
):
    tiles = cpad.shape[0] // LANES
    batch_total = n * batch
    coef = 1.0 / (2 * batch_total * TEMPERATURE)
    me = lax.axis_index("data")
    own = pl.ds(pl.multiple_of(me * batch, batch), batch)
    codes_hbm = (codes1_hbm, codes2_hbm)
    dz_hbm = (dz1_hbm, dz2_hbm)

    logs = lse_sum[0]
    for d in range(1, n):
        logs = logs + lse_sum[d]
    total = jnp.sum(small[2]) * (1.0 / TEMPERATURE) - jnp.sum(logs) * (1.0 / LANES)
    loss[0, 0] = total * (-1.0 / (2 * batch_total))
    pltpu.make_async_copy(loss, loss_hbm, out_sem.at[5]).start()

    pairs = tiles // 2
    deep = 2 * batch

    def cols_of(jj):
        return pl.ds(jj * 2 * LANES, min(2 * LANES, protos - jj * 2 * LANES))

    def body(acc, dz_acc):
        for ref in (*acc[0], *acc[1], *dz_acc):
            pltpu.matmul_pop(ref)

        def scaled(v, j, sl):
            t = aall[v, j, sl, :]
            return t if v == 0 else t * small[v, j:j + 1, :]

        def tiles_of(big, v):
            for d in range(0, n, 2):
                sl = pl.ds(d * batch, deep)
                scale = rinv[v, sl, :]
                lhs = zt[:, pl.ds((1 - v) * n * batch + d * batch, deep)]
                reg = (d // 2) % 2
                for unit in range(2):
                    g = [pall[1 - v, j, sl, :] - scaled(v, j, sl) * scale
                         for j in (4 * big + 2 * unit, 4 * big + 2 * unit + 1)]
                    pltpu.matmul_push_rhs(jnp.concatenate(g, axis=1), staging_register=reg, mxu_index=unit)
                    pltpu.matmul_acc_lhs(acc[big][unit], lhs, load_staged_rhs=reg)

        def own_part(jj):
            lhs = []
            for v in range(2):
                g = []
                for h in range(2):
                    j = 2 * jj + h
                    part = min(LANES, protos - j * LANES)
                    q = scaled(v, j, own) * rinv[v, own, :]
                    g.append(pall[1 - v, j, own, :] - q)
                    codes[v, pl.ds(j * LANES, part), :] = (q * (1.0 / coef)).T[:part]
                lhs.insert(0, jnp.concatenate(g, axis=1))
            c = cpad[pl.ds(jj * 2 * LANES, 2 * LANES), :].astype(F32)
            pltpu.matmul_push_rhs(jnp.concatenate([c, c], axis=1), staging_register=0, mxu_index=jj % 2)
            pltpu.matmul_acc_lhs(dz_acc[jj % 2], jnp.concatenate(lhs, axis=0), load_staged_rhs=0)

        def drain(big):
            for unit in range(2):
                cols = cols_of(2 * big + unit)
                gp[cols, :] = pltpu.matmul_pop(acc[big][unit]).T[:cols.size]

        def send(big):
            for first in range(4 * big * LANES, 4 * (big + 1) * LANES, LANES // 2):
                cols = pl.ds(first, max(0, min(LANES // 2, protos - first)))
                if cols.size:
                    pltpu.make_async_copy(gp.at[cols], gp_hbm.at[cols], out_sem.at[4]).start()

        def send_codes(big):
            for jj in (2 * big, 2 * big + 1):
                cols = cols_of(jj)
                for v in range(2):
                    pltpu.make_async_copy(codes.at[v, cols], codes_hbm[v].at[cols], out_sem.at[v]).start()

        own_part(0)
        own_part(1)
        send_codes(0)
        tiles_of(0, 0)
        tiles_of(0, 1)
        own_part(2)
        own_part(3)
        send_codes(1)
        tiles_of(1, 0)
        drain(0)
        send(0)
        o = pltpu.matmul_pop(dz_acc[0]) + pltpu.matmul_pop(dz_acc[1])
        for v in range(2):
            dz[v] = o[v * batch:(v + 1) * batch, :LANES]
            pltpu.make_async_copy(dz.at[v], dz_hbm[v], out_sem.at[2 + v]).start()
        tiles_of(1, 1)
        drain(1)
        send(1)

    def acc_of(rows):
        return tuple(pltpu.ACC(unit)((rows, 2 * LANES), F32) for unit in range(2))

    pl.run_scoped(body, (acc_of(LANES), acc_of(LANES)), acc_of(deep))

    for v in range(2):
        pltpu.make_async_copy(codes.at[v, pl.ds(0, protos)], codes_hbm[v], out_sem.at[v]).wait()
        pltpu.make_async_copy(dz.at[v], dz_hbm[v], out_sem.at[2 + v]).wait()
    pltpu.make_async_copy(gp.at[pl.ds(0, protos)], gp_hbm, out_sem.at[4]).wait()
    pltpu.make_async_copy(loss, loss_hbm, out_sem.at[5]).wait()


def solution(mesh):
    n = mesh.shape["data"]

    def local_step(z_one, z_two, protos, queue_one, queue_two):
        k, width = protos.shape
        batch, queue = z_one.shape[0], queue_one.shape[0]
        rows = batch + queue
        pad = (k + 255) // 256 * 256
        tiles = pad // LANES
        anywhere = pl.BlockSpec(memory_space=pl.ANY)
        sem = pltpu.SemaphoreType.DMA
        vmem = pl.BlockSpec(memory_space=pltpu.VMEM)
        whole = n * batch
        shared = pl.pallas_call(
            functools.partial(sums_kernel, n, k, batch, queue),
            out_shape=(
                pltpu.VMEM((2, tiles, whole, LANES), F32),
                pltpu.VMEM((2, tiles, whole, LANES), F32),
                pltpu.VMEM((2, whole, LANES), F32),
                pltpu.VMEM((width, 2 * whole), F32),
                pltpu.VMEM((pad, width), BF16),
                pltpu.VMEM((4, tiles, LANES), F32),
                pltpu.VMEM((n, 8, LANES), F32),
            ),
            in_specs=[anywhere] * 5,
            out_specs=(vmem,) * 7,
            scratch_shapes=[
                pltpu.VMEM((2, 2, rows, width), BF16),
                pltpu.VMEM((n, 2, batch, width), BF16),
                pltpu.VMEM((2, tiles, whole, LANES), F32),
                pltpu.VMEM((2, tiles, 2 * rows, LANES), F32),
                pltpu.VMEM((2, 8 * tiles, LANES), F32),
                pltpu.VMEM((ROUNDS, 2, n, tiles, LANES), F32),
                sem((4,)),
                sem((2, 2)),
                sem((5,)),
                sem((2,)),
            ],
            compiler_params=pltpu.CompilerParams(
                collective_id=0, has_side_effects=True, vmem_limit_bytes=26 << 20),
            name="sums",
        )(*(pltpu.with_memory_space_constraint(x, pltpu.HBM) for x in (z_one, z_two, protos, queue_one, queue_two)))
        codes_one, codes_two, loss, dz_one, dz_two, grad_protos = pl.pallas_call(
            functools.partial(grads_kernel, n, k, batch),
            out_shape=(
                jax.ShapeDtypeStruct((k, batch), F32),
                jax.ShapeDtypeStruct((k, batch), F32),
                jax.ShapeDtypeStruct((1, 1), F32),
                jax.ShapeDtypeStruct((batch, width), F32),
                jax.ShapeDtypeStruct((batch, width), F32),
                jax.ShapeDtypeStruct((k, width), F32),
            ),
            in_specs=[vmem] * 7,
            out_specs=(anywhere,) * 6,
            scratch_shapes=[
                pltpu.VMEM((2, pad, batch), F32),
                pltpu.VMEM((pad, width), F32),
                pltpu.VMEM((2, batch, width), F32),
                pltpu.SMEM((1, 1), F32),
                sem((6,)),
            ],
            compiler_params=pltpu.CompilerParams(vmem_limit_bytes=14 << 20),
            name="grads",
        )(*shared)
        return codes_one.T, codes_two.T, loss[0, 0], dz_one, dz_two, grad_protos

    row_spec = P("data", None)
    full_spec = P(None, None)
    return jax.shard_map(
        local_step,
        mesh=mesh,
        in_specs=(row_spec, row_spec, full_spec, row_spec, row_spec),
        out_specs=(row_spec, row_spec, P(), row_spec, row_spec, full_spec),
        check_vma=False,
    )
```
